256 devices in a mesh: rows: 64 (over y, z, core), cols: 4 (over x).
Axes of the slice: x: 4, y: 4, z: 8, core: 2. Of those that a mesh axis runs over, the one named last changes fastest.
Arguments:
- panel: float32 [131072, 256], P(('rows', 'cols')), may hold values from -17 to 17, as said below
- trailing: float32 [131072, 2048], P('rows', 'cols'), may hold values from -6 to 6
Outputs:
- rfactor: float32 [256, 256], replicated
- projected: float32 [256, 2048], P(None, 'cols')
- updated: float32 [131072, 2048], P('rows', 'cols')
The draws below stay inside these ranges and needn't reach their ends.
Inputs may be any that keep to these rules, and one draw needn't show every extreme that they name: The panel has full column rank with a moderate condition number (under 100); each column has its own scale and a part shared by all columns.
All inputs are finite; a program needn't handle non-finite values.
Results may differ from the reference program's by a relative error of at most 0.000078.
Values sent between devices are 32-bit elements; how exact they have to be, the bound alone decides.
A program may use at most 64 MiB of HBM per device.

```python
import jax
import jax.numpy as jnp
from jax import lax

PANEL = 256
TRAIL = 2048
ROWS = 131072
PIECE = 512


def draw_panel(key, part):
    keys = jax.random.split(jax.random.fold_in(key, 17), 5)
    noise = jnp.clip(jax.random.normal(keys[0], (ROWS, PANEL), jnp.float32), -6.0, 6.0)
    pieces = ROWS // PIECE
    piece_of_row = jnp.arange(ROWS) // PIECE
    scales = jnp.exp(jax.random.uniform(keys[1], (PANEL,), jnp.float32, jnp.log(0.5), jnp.log(2.0)))
    common = jnp.clip(jax.random.normal(keys[2], (ROWS,), jnp.float32), -5.0, 5.0)
    tilt = jax.random.uniform(keys[3], (PANEL,), jnp.float32, -0.7, 0.7)
    boosted = jax.random.randint(keys[4], (pieces,), 0, PANEL)
    column_ids = jnp.arange(PANEL)
    boost = 1.0 + 5.0 * (column_ids[None, :] == boosted[piece_of_row][:, None]).astype(jnp.float32)
    values = (noise * scales[None, :] + common[:, None] * tilt[None, :]) * boost
    return (values / jnp.sqrt(jnp.float32(ROWS))).astype(jnp.float32)


def levels(stream_key, shape, cuts, smallest, largest):
    level, own = 1.0, jax.random.fold_in(stream_key, 6)
    for axis_at, parts in cuts:
        draws = jnp.exp(jax.random.uniform(jax.random.fold_in(own, axis_at), (parts,), jnp.float32, smallest / len(cuts), largest / len(cuts)))
        level = level * jnp.repeat(draws, shape[axis_at] // parts).reshape([-1 if axis == axis_at else 1 for axis in range(len(shape))])
    return level


def gaussian(stream_key, dims, deviation, bound, cuts=(), held_as=jnp.bfloat16):
    entries = deviation * jax.random.normal(stream_key, dims, jnp.float32)
    if cuts:
        entries = entries * levels(stream_key, dims, cuts, -0.22, 0.18)
    return jnp.clip(entries, -bound, bound).astype(held_as)


def setup_inputs(seed: int = 0) -> dict:
    arg_keys = jax.random.split(jax.random.key(seed), 3)
    return {
        "panel": draw_panel(jax.random.fold_in(arg_keys[2], 71), 0),
        "trailing": gaussian(arg_keys[1], (ROWS, TRAIL), 1.0, 6.0, ((0, 64), (1, 4)), jnp.float32),
    }


def inner(left, right):
    return lax.dot_general(left.astype(jnp.float32), right.astype(jnp.float32), (((0,), (0,)), ((), ())), precision=lax.Precision.HIGHEST, preferred_element_type=jnp.float32)

def reference(panel, trailing):
    gram = inner(panel, panel)
    rfactor = jnp.linalg.cholesky(gram).T
    basis = jax.scipy.linalg.solve_triangular(rfactor.T, panel.T, lower=True).T
    cross = inner(panel, trailing)
    projected = jax.scipy.linalg.solve_triangular(rfactor.T, cross, lower=True)
    updated = trailing - jnp.dot(basis.astype(jnp.float32), projected.astype(jnp.float32), precision=lax.Precision.HIGHEST, preferred_element_type=jnp.float32)
    return (rfactor, projected, updated)
```

```python
import functools

import jax
import jax.numpy as jnp
from jax import lax
from jax.experimental import pallas as pl
from jax.experimental.pallas import tpu as pltpu
from jax.sharding import PartitionSpec as P

MESH = pl.DeviceIdType.MESH
HIGHEST = lax.Precision.HIGHEST
F32 = jnp.float32


def dot(left, right):
    return jnp.dot(left, right, precision=HIGHEST, preferred_element_type=F32)


class Place:
    def __init__(self):
        rows = lax.axis_index("rows")
        self.x = lax.axis_index("cols")
        self.core = lax.rem(rows, 2)
        self.z = lax.rem(rows // 2, 8)
        self.y = rows // 16

    def at(self, y=0, z=0, core=0, x=0):
        there = lax.rem(self.y + y, 4) * 16 + lax.rem(self.z + z, 8) * 2 + lax.rem(self.core + core, 2)
        return (there, lax.rem(self.x + x, 4))


def send(src, dst, send_sem, recv_sem, device):
    copy = pltpu.make_async_remote_copy(
        src_ref=src, dst_ref=dst, send_sem=send_sem, recv_sem=recv_sem, device_id=device, device_id_type=MESH
    )
    copy.start()
    return copy


class Reduction:
    def __init__(self, place, refs, over_x):
        self.place, self.over_x = place, over_x
        self.part, self.from_core, self.s1, self.from_y, self.s2, self.from_z, self.s3, self.from_x, self.full = refs[:9]
        self.send_sem, self.recv_sem = refs[9:]
        self.copies = []
        self.used = 0

    def send(self, src, dst, device):
        copy = send(src, dst, self.send_sem.at[self.used], self.recv_sem.at[self.used], device)
        self.used += 1
        self.copies.append(copy)
        return copy

    def start_core(self):
        p = self.place
        self.c1 = self.send(self.part.at[pl.ds(16 * (1 - p.core), 16)], self.from_core, p.at(core=1))

    def start_y(self):
        p = self.place
        self.c1.wait_recv()
        self.s1[...] = self.part[pl.ds(16 * p.core, 16)] + self.from_core[...]
        self.c2 = [
            self.send(self.s1.at[pl.ds(4 * lax.rem(p.y + d, 4), 4)], self.from_y.at[d - 1], p.at(y=d)) for d in (2, 1, 3)
        ]

    def start_z(self):
        p = self.place
        for c in self.c2:
            c.wait_recv()
        self.s2[...] = (self.s1[pl.ds(4 * p.y, 4)] + self.from_y[0]) + (self.from_y[1] + self.from_y[2])
        self.c3 = []
        for d in (4, 3, 5, 2, 6, 1, 7):
            there = lax.rem(p.z + d, 8)
            self.c3.append(self.send(self.s2.at[there // 2, lax.rem(there, 2)], self.from_z.at[d - 1], p.at(z=d)))

    def end_z(self):
        p = self.place
        for c in self.c3:
            c.wait_recv()
        total = self.s2[p.z // 2, lax.rem(p.z, 2)]
        for d in range(7):
            total = total + self.from_z[d]
        return total

    def start_x(self):
        p = self.place
        self.s3[...] = self.end_z()
        self.c4 = [self.send(self.s3, self.from_x.at[p.x], p.at(x=d)) for d in (2, 1, 3)]
        self.from_x[p.x] = self.s3[...]

    def start_gather_z(self):
        p = self.place
        group, half = 16 * p.core + 4 * p.y + p.z // 2, lax.rem(p.z, 2)
        if self.over_x:
            for c in self.c4:
                c.wait_recv()
            self.full[group, half] = (self.from_x[0] + self.from_x[1]) + (self.from_x[2] + self.from_x[3])
        else:
            self.full[group, half] = self.end_z()
        mine = self.full.at[group, half]
        self.c5 = [self.send(mine, mine, p.at(z=d)) for d in (4, 3, 5, 2, 6, 1, 7)]

    def start_gather_y(self):
        p = self.place
        for c in self.c5:
            c.wait_recv()
        mine = self.full.at[pl.ds(16 * p.core + 4 * p.y, 4)]
        self.c6 = [self.send(mine, mine, p.at(y=d)) for d in (2, 1, 3)]
        self.c7 = [self.send(mine, mine, p.at(core=1))]

    def start_gather_core(self):
        p = self.place
        for c, d in zip(self.c6, (2, 1, 3)):
            c.wait_recv()
            theirs = self.full.at[pl.ds(16 * p.core + 4 * lax.rem(p.y + 4 - d, 4), 4)]
            self.c7.append(self.send(theirs, theirs, p.at(core=1)))

    def finish(self):
        for c in self.c7:
            c.wait_recv()

    def drain(self):
        for c in self.copies:
            c.wait_send()


def halves(ref, width):
    return jnp.concatenate([ref[:, h].reshape(256, width // 2) for h in range(2)], axis=1)


def reduce_kernel(panel, trailing, block, gram, cross, held, load_sem, side_send, side_recv, *rest):
    p = Place()
    g = Reduction(p, (*rest[:8], gram, *rest[8:10]), True)
    t = Reduction(p, (*rest[10:18], cross, *rest[18:20]), False)

    own = pltpu.make_async_copy(panel, block.at[p.x], load_sem.at[0])
    own.start()
    load = pltpu.make_async_copy(trailing, held, load_sem.at[1])
    load.start()

    barrier = pltpu.get_barrier_semaphore()
    peers = [p.at(core=1)] + [p.at(y=d) for d in (1, 2, 3)] + [p.at(z=d) for d in range(1, 8)] + [p.at(x=d) for d in (1, 2, 3)]
    for peer in peers:
        pl.semaphore_signal(barrier, inc=1, device_id=peer, device_id_type=MESH)
    pl.semaphore_wait(barrier, len(peers))

    own.wait()
    steps = (1, 3)
    direct = [[None, None], [None, None]]
    for n in range(2):
        for side in range(2):
            half = n if side == 0 else 1 - n
            rows = block.at[p.x, pl.ds(256 * half, 256)]
            at = 2 * side + half
            direct[side][half] = send(rows, rows, side_send.at[at], side_recv.at[at], p.at(x=steps[side]))

    mine = block[p.x]
    product = dot(mine.T, mine)
    for h in range(2):
        g.part[:, h] = product[:, 128 * h : 128 * h + 128].reshape(32, 8, 128)
    g.start_core()

    load.wait()

    def add_cross(x, first):
        product = dot(block[x].T, held[pl.ds(512 * x, 512), :])
        for h in range(2):
            term = product[:, 256 * h : 256 * h + 256].reshape(32, 8, 256)
            t.part[:, h] = term if first else t.part[:, h] + term

    add_cross(p.x, True)
    g.start_y()
    g.start_z()
    g.start_x()
    relays = []
    for side in range(2):
        direct[side][side].wait_recv()
        source = lax.rem(p.x + steps[1 - side], 4)
        rows = block.at[source, pl.ds(256 * side, 256)]
        relays.append(send(rows, rows, side_send.at[4 + side], side_recv.at[4 + side], p.at(x=steps[side])))
    for side in range(2):
        direct[side][1 - side].wait_recv()
        add_cross(lax.rem(p.x + steps[1 - side], 4), False)
    g.start_gather_z()
    for r in relays:
        r.wait_recv()
    add_cross(lax.rem(p.x + 2, 4), False)
    t.start_core()
    g.start_gather_y()
    t.start_y()
    g.start_gather_core()
    t.start_z()
    g.finish()
    t.start_gather_z()
    t.start_gather_y()
    t.start_gather_core()
    t.finish()
    for side in range(2):
        for copy in direct[side]:
            copy.wait_send()
        relays[side].wait_send()
    g.drain()
    t.drain()


def scratch(width):
    w = width // 2
    vm = lambda *shape: pltpu.VMEM((*shape, 8, w), F32)
    return [
        vm(32, 2), vm(16, 2), vm(16, 2), vm(3, 4, 2), vm(4, 2), vm(7), vm(), vm(4),
        pltpu.SemaphoreType.DMA((28,)), pltpu.SemaphoreType.DMA((28,)),
    ]


def gather_and_reduce(panel, trailing):
    whole = pl.BlockSpec(memory_space=pltpu.VMEM)
    return pl.pallas_call(
        reduce_kernel,
        out_shape=(
            jax.ShapeDtypeStruct((4, 512, 256), F32),
            jax.ShapeDtypeStruct((32, 2, 8, 128), F32),
            jax.ShapeDtypeStruct((32, 2, 8, 256), F32),
        ),
        in_specs=[pl.BlockSpec(memory_space=pltpu.HBM)] * 2,
        out_specs=(whole,) * 3,
        scratch_shapes=[
            pltpu.VMEM((2048, 512), F32),
            pltpu.SemaphoreType.DMA((2,)),
            pltpu.SemaphoreType.DMA((6,)),
            pltpu.SemaphoreType.DMA((6,)),
            *scratch(256),
            *scratch(512),
        ],
        compiler_params=pltpu.CompilerParams(collective_id=0, has_side_effects=True, vmem_limit_bytes=32 << 20),
    )(panel, trailing)


def row_of(x, j):
    return jnp.broadcast_to(x[j : j + 1, :], x.shape)


def lane_of(x, at):
    return jnp.take_along_axis(x, at, axis=1)


def eight_pivots(k, c, first, a, r, inv):
    sub = lax.broadcasted_iota(jnp.int32, (8, 128), 0)
    lane = lax.broadcasted_iota(jnp.int32, (8, 128), 1)
    start = (k - 16 * c) * 8
    rel = lane - start
    inside = (rel >= 0) & (rel < 8)
    ats = [jnp.zeros((8, 128), jnp.int32) + (start + j) for j in range(8)]
    work = [a[k, h] for h in range(2)]
    d = work[c]
    cols = [lane_of(d, at) for at in ats]
    work[c] = jnp.where(inside, (rel == sub).astype(F32), d)
    work.append(d)
    outs = [jnp.zeros((8, 128), F32) for _ in work]
    for j in range(8):
        pivot = row_of(cols[j], j)
        inverse = 1.0 / pivot
        root = lax.rsqrt(pivot)
        here = sub == j
        for m in range(j + 1, 8):
            term = row_of(cols[m], j) * inverse
            cols[m] = jnp.where(here, term, cols[m] - cols[j] * term)
        for w in range(3):
            row = row_of(work[w], j)
            outs[w] = jnp.where(here, row * root, outs[w])
            term = row * inverse
            work[w] = work[w] - cols[j] * term if w == 2 else jnp.where(here, term, work[w] - cols[j] * term)
    zero = jnp.zeros((8, 128), F32)
    for h in range(2):
        if h == c:
            r[k, h] = jnp.where(rel >= sub, outs[2], 0.0)
            inv[k, h] = jnp.where(rel <= sub, outs[h], 0.0)
        else:
            r[k, h] = outs[h] if h > c else zero
            inv[k, h] = outs[h] if h < c else zero
    rows = [[row_of(work[h], j) for j in range(8)] for h in range(2)]
    for group in range(first, 32):
        old = [a[group, h] for h in range(2)]
        new = list(old)
        new[c] = jnp.where(inside, 0.0, old[c])
        for j in range(8):
            multiplier = lane_of(old[c], ats[j])
            for h in range(2):
                new[h] = new[h] - multiplier * rows[h][j]
        for h in range(2):
            a[group, h] = new[h]


def factor_quarter(q, a, r, inv):
    def step(i, carry):
        eight_pivots(8 * q + i, q // 2, 8 * q, a, r, inv)
        return carry

    lax.fori_loop(0, 8, step, 0)


def factor_kernel(gram, cross, rfactor, projected, weight_high, weight_low, a, r, inv):
    a[...] = gram[...]
    for q in range(4):
        factor_quarter(q, a, r, inv)
    rfactor[...] = halves(r, 256)
    inverse = halves(inv, 256)
    proj = dot(inverse, halves(cross, 512))
    projected[...] = proj
    weight = dot(inverse.T, proj)
    high = weight.astype(jnp.bfloat16)
    weight_high[...] = high
    weight_low[...] = (weight - high.astype(F32)).astype(jnp.bfloat16)


def factor(gram, cross):
    held = pltpu.VMEM((32, 2, 8, 128), F32)
    return pl.pallas_call(
        factor_kernel,
        out_shape=(
            jax.ShapeDtypeStruct((256, 256), F32),
            jax.ShapeDtypeStruct((256, 512), F32),
            jax.ShapeDtypeStruct((256, 512), jnp.bfloat16),
            jax.ShapeDtypeStruct((256, 512), jnp.bfloat16),
        ),
        scratch_shapes=[held, held, held],
        compiler_params=pltpu.CompilerParams(vmem_limit_bytes=16 << 20),
    )(gram, cross)


def update_kernel(trailing, block, weight_high, weight_low, updated):
    x = block[...]
    high = x.astype(jnp.bfloat16)
    low = (x - high.astype(F32)).astype(jnp.bfloat16)
    mul = functools.partial(jnp.dot, preferred_element_type=F32)
    updated[...] = trailing[...] - (mul(high, weight_high[...]) + (mul(high, weight_low[...]) + mul(low, weight_high[...])))


def update(trailing, block, weight_high, weight_low):
    rows = 512
    tile = pl.BlockSpec((rows, 512), lambda i: (i, 0))
    fixed = pl.BlockSpec((256, 512), lambda i: (0, 0))
    return pl.pallas_call(
        update_kernel,
        grid=(2048 // rows,),
        out_shape=jax.ShapeDtypeStruct((2048, 512), F32),
        in_specs=[tile, pl.BlockSpec((rows, 256), lambda i: (i, 0)), fixed, fixed],
        out_specs=tile,
        compiler_params=pltpu.CompilerParams(vmem_limit_bytes=24 << 20),
    )(trailing, block, weight_high, weight_low)


def shards(panel, trailing):
    block, gram, cross = gather_and_reduce(panel, trailing)
    rfactor, projected, high, low = factor(gram, cross)
    return rfactor, projected, update(trailing, block.reshape(2048, 256), high, low)


def solution(mesh):
    return jax.shard_map(
        shards,
        mesh=mesh,
        in_specs=(P(("rows", "cols"), None), P("rows", "cols")),
        out_specs=(P(), P(None, "cols"), P("rows", "cols")),
        check_vma=False,
    )
```

```python
import functools

import jax
import jax.numpy as jnp
from jax import lax
from jax.experimental import pallas as pl
from jax.experimental.pallas import tpu as pltpu
from jax.sharding import PartitionSpec as P

MESH = pl.DeviceIdType.MESH
HIGHEST = lax.Precision.HIGHEST
F32 = jnp.float32


def dot(left, right):
    return jnp.dot(left, right, precision=HIGHEST, preferred_element_type=F32)


class Place:
    def __init__(self):
        rows = lax.axis_index("rows")
        self.x = lax.axis_index("cols")
        self.core = lax.rem(rows, 2)
        self.z = lax.rem(rows // 2, 8)
        self.y = rows // 16

    def at(self, y=0, z=0, core=0, x=0):
        there = lax.rem(self.y + y, 4) * 16 + lax.rem(self.z + z, 8) * 2 + lax.rem(self.core + core, 2)
        return (there, lax.rem(self.x + x, 4))


def send(src, dst, send_sem, recv_sem, device):
    copy = pltpu.make_async_remote_copy(
        src_ref=src, dst_ref=dst, send_sem=send_sem, recv_sem=recv_sem, device_id=device, device_id_type=MESH
    )
    copy.start()
    return copy


class Reduction:
    def __init__(self, place, refs, over_x):
        self.place, self.over_x = place, over_x
        self.part, self.from_core, self.s1, self.from_y, self.s2, self.from_z, self.s3, self.from_x, self.full = refs[:9]
        self.send_sem, self.recv_sem = refs[9:]
        self.groups, self.across = self.part.shape[:2]
        self.half, self.eighth = self.groups // 2, self.groups // 8
        self.copies = []

    def send(self, src, dst, device):
        used = len(self.copies)
        copy = send(src, dst, self.send_sem.at[used], self.recv_sem.at[used], device)
        self.copies.append(copy)
        return copy

    def start_core(self):
        p = self.place
        self.c1 = self.send(self.part.at[pl.ds(self.half * (1 - p.core), self.half)], self.from_core, p.at(core=1))

    def start_y(self):
        p, n = self.place, self.eighth
        self.c1.wait_recv()
        self.s1[...] = self.part[pl.ds(self.half * p.core, self.half)] + self.from_core[...]
        self.c2 = [self.send(self.s1.at[pl.ds(n * lax.rem(p.y + d, 4), n)], self.from_y.at[d - 1], p.at(y=d)) for d in (2, 1, 3)]

    def start_z(self):
        p, n = self.place, self.eighth
        for c in self.c2:
            c.wait_recv()
        self.s2[...] = (self.s1[pl.ds(n * p.y, n)] + self.from_y[0]) + (self.from_y[1] + self.from_y[2])
        self.c3 = []
        for d in (4, 3, 5, 2, 6, 1, 7):
            there = lax.rem(p.z + d, 8)
            self.c3.append(self.send(self.s2.at[there // self.across, lax.rem(there, self.across)], self.from_z.at[d - 1], p.at(z=d)))

    def end_z(self):
        p = self.place
        for c in self.c3:
            c.wait_recv()
        f = self.from_z
        total = self.s2[p.z // self.across, lax.rem(p.z, self.across)]
        return ((total + f[0]) + (f[1] + f[2])) + ((f[3] + f[4]) + (f[5] + f[6]))

    def start_x(self):
        p = self.place
        self.s3[...] = self.end_z()
        self.c4 = [self.send(self.s3, self.from_x.at[p.x], p.at(x=d)) for d in (2, 1, 3)]
        self.from_x[p.x] = self.s3[...]

    def start_gather_z(self):
        p = self.place
        group, across = self.half * p.core + self.eighth * p.y + p.z // self.across, lax.rem(p.z, self.across)
        if self.over_x:
            for c in self.c4:
                c.wait_recv()
            self.full[group, across] = (self.from_x[0] + self.from_x[1]) + (self.from_x[2] + self.from_x[3])
        else:
            self.full[group, across] = self.end_z()
        mine = self.full.at[group, across]
        self.c5 = [self.send(mine, mine, p.at(z=d)) for d in (4, 3, 5, 2, 6, 1, 7)]

    def block(self, y):
        return self.full.at[pl.ds(self.half * self.place.core + self.eighth * y, self.eighth)]

    def start_gather_y(self):
        p = self.place
        for c in self.c5:
            c.wait_recv()
        mine = self.block(p.y)
        self.c6 = [self.send(mine, mine, p.at(y=d)) for d in (2, 1, 3)]
        self.c7 = [self.send(mine, mine, p.at(core=1))]

    def start_gather_core(self):
        p = self.place
        for c, d in zip(self.c6, (2, 1, 3)):
            c.wait_recv()
            theirs = self.block(lax.rem(p.y + 4 - d, 4))
            self.c7.append(self.send(theirs, theirs, p.at(core=1)))

    def finish(self):
        for c in self.c7:
            c.wait_recv()

    def drain(self):
        for c in self.copies:
            c.wait_send()


def tiled(matrix):
    n = matrix.shape[0] // 8
    return [matrix[:, 128 * h : 128 * h + 128].reshape(n, 8, 128) for h in range(matrix.shape[1] // 128)]


def whole(ref):
    n, m = ref.shape[:2]
    return jnp.concatenate([ref[:, h].reshape(8 * n, 128) for h in range(m)], axis=1)


def row_of(x, j):
    return jnp.broadcast_to(x[j : j + 1, :], x.shape)


def lane_of(x, at):
    return jnp.take_along_axis(x, at, axis=1)


def eight_pivots(k, base, a, r, inv):
    sub = lax.broadcasted_iota(jnp.int32, (8, 128), 0)
    lane = lax.broadcasted_iota(jnp.int32, (8, 128), 1)
    rel = [lane + (128 * h - 8 * k) for h in range(2)]
    inside = [(x >= 0) & (x < 8) for x in rel]
    c = k // 16
    start = 8 * lax.rem(k, 16)
    ats = [jnp.zeros((8, 128), jnp.int32) + (start + j) for j in range(8)]
    d = a[k, c]
    cols = [lane_of(d, at) for at in ats]
    work = [jnp.where(inside[h], (rel[h] == sub).astype(F32), a[k, h]) for h in range(2)] + [d]
    outs = [jnp.zeros((8, 128), F32) for _ in work]
    for j in range(8):
        here = sub == j
        root = lax.rsqrt(row_of(cols[j], j))
        scaled = cols[j] * root
        for m in range(j + 1, 8):
            term = row_of(cols[m], j) * root
            cols[m] = jnp.where(here, term * root, cols[m] - scaled * term)
        for w in range(3):
            term = row_of(work[w], j) * root
            outs[w] = jnp.where(here, term, outs[w])
            rest = work[w] - scaled * term
            work[w] = rest if w == 2 else jnp.where(here, term * root, rest)
    for h in range(2):
        r[k, h] = jnp.where(rel[h] >= 8, outs[h], jnp.where(inside[h] & (rel[h] >= sub), outs[2], 0.0))
        inv[k, h] = jnp.where(rel[h] <= sub, outs[h], 0.0)
    rows = [[row_of(work[h], j) for j in range(8)] for h in range(2)]
    source = [a[base + g, c] for g in range(8)]
    new = [[jnp.where(inside[h], 0.0, a[base + g, h]) for h in range(2)] for g in range(8)]
    for j in range(8):
        for g in range(8):
            multiplier = lane_of(source[g], ats[j])
            for h in range(2):
                new[g][h] = new[g][h] - multiplier * rows[h][j]
    for g in range(8):
        for h in range(2):
            a[base + g, h] = new[g][h]


def take_out(s, a, r, inv):
    base = 8 * s
    rows = lambda ref, h: ref[pl.ds(base, 8), h].reshape(64, 128)
    right = []
    for h in range(2):
        col = lax.broadcasted_iota(jnp.int32, (64, 128), 1) + 128 * h
        right.append(jnp.where(col < 64 * (s + 1), rows(inv, h), rows(r, h)))
    right = jnp.concatenate(right, axis=1)
    for half in range((s + 1) // 2, 2):
        product = tiled(dot(rows(r, half).T, right))
        for h in range(2):
            col = lax.broadcasted_iota(jnp.int32, (16, 8, 128), 2) + 128 * h
            old = a[pl.ds(16 * half, 16), h]
            a[pl.ds(16 * half, 16), h] = jnp.where((col >= 64 * s) & (col < 64 * (s + 1)), 0.0, old) - product[h]


def factor_part(eighth, a, r, inv):
    s = eighth // 2

    def step(i, carry):
        eight_pivots(4 * eighth + i, 8 * s, a, r, inv)
        return carry

    lax.fori_loop(0, 4, step, 0)
    if eighth % 2 and s < 3:
        take_out(s, a, r, inv)


def split(x):
    high = x.astype(jnp.bfloat16)
    return high, (x - high.astype(F32)).astype(jnp.bfloat16)


def main_kernel(
    panel, trailing, block_high, block_low, rfactor, projected, weight_high, weight_low,
    block, held, a, inv, r, load_sem, side_send, side_recv, *rest
):
    p = Place()
    g = Reduction(p, rest[:11], True)
    t = [Reduction(p, rest[11 + 11 * q : 22 + 11 * q], False) for q in range(2)]

    own = pltpu.make_async_copy(panel, block.at[p.x], load_sem.at[0])
    own.start()
    load = pltpu.make_async_copy(trailing, held, load_sem.at[1])
    load.start()

    barrier = pltpu.get_barrier_semaphore()
    peers = [p.at(core=1)] + [p.at(y=d) for d in (1, 2, 3)] + [p.at(z=d) for d in range(1, 8)] + [p.at(x=d) for d in (1, 2, 3)]
    for peer in peers:
        pl.semaphore_signal(barrier, inc=1, device_id=peer, device_id_type=MESH)
    pl.semaphore_wait(barrier, len(peers))
    own.wait()

    steps = (1, 3)
    x_copies = []

    def side_copy(source, q, half, side, slot):
        rows = block.at[source, pl.ds(256 * half, 256), pl.ds(128 * q, 128)]
        at = 6 * q + 2 * slot + side
        copy = send(rows, rows, side_send.at[at], side_recv.at[at], p.at(x=steps[side]))
        x_copies.append(copy)
        return copy

    def direct(q, n):
        return [side_copy(p.x, q, n if side == 0 else 1 - n, side, n) for side in range(2)]

    def relay(q, arrived):
        copies = []
        for side in range(2):
            arrived[side].wait_recv()
            copies.append(side_copy(lax.rem(p.x + steps[1 - side], 4), q, side, side, 2))
        return copies

    def wait(copies):
        for copy in copies:
            copy.wait_recv()

    def add_cross(q, step, first=False):
        x = lax.rem(p.x + step, 4)
        terms = tiled(dot(block[x, :, 128 * q : 128 * q + 128].T, held[pl.ds(512 * x, 512), :]))
        for h in range(4):
            t[q].part[:, h] = terms[h] if first else t[q].part[:, h] + terms[h]

    first0 = direct(0, 0)
    second0 = direct(0, 1)
    mine = block[p.x]
    for h, tile in enumerate(tiled(dot(mine.T, mine))):
        g.part[:, h] = tile
    g.start_core()
    load.wait()
    add_cross(0, 0, True)
    g.start_y()
    relay0 = relay(0, first0)
    first1 = direct(1, 0)
    add_cross(1, 0, True)
    g.start_z()
    wait(second0)
    add_cross(0, 1)
    add_cross(0, 3)
    g.start_x()
    second1 = direct(1, 1)
    wait(relay0)
    add_cross(0, 2)
    t[0].start_core()
    t[0].start_y()
    relay1 = relay(1, first1)
    g.start_gather_z()
    wait(second1)
    add_cross(1, 1)
    add_cross(1, 3)
    t[0].start_z()
    g.start_gather_y()
    wait(relay1)
    add_cross(1, 2)
    t[1].start_core()
    for x in range(4):
        rows = pl.ds(512 * x, 512)
        block_high[rows, :], block_low[rows, :] = split(block[x])
    g.start_gather_core()
    t[1].start_y()
    g.finish()
    a[...] = g.full[...]
    factor_part(0, a, r, inv)
    t[0].start_gather_z()
    factor_part(1, a, r, inv)
    t[1].start_z()
    factor_part(2, a, r, inv)
    factor_part(3, a, r, inv)
    t[0].start_gather_y()
    factor_part(4, a, r, inv)
    t[1].start_gather_z()
    factor_part(5, a, r, inv)
    t[0].start_gather_core()
    factor_part(6, a, r, inv)
    factor_part(7, a, r, inv)
    t[1].start_gather_y()
    rfactor[...] = whole(r)
    inverse = whole(inv)
    t[0].finish()
    proj = dot(inverse[:, :128], whole(t[0].full))
    t[1].start_gather_core()
    t[1].finish()
    proj = proj + dot(inverse[:, 128:], whole(t[1].full))
    projected[...] = proj
    weight_high[...], weight_low[...] = split(dot(inverse.T, proj))
    for copy in x_copies:
        copy.wait_send()
    for reduction in (g, *t):
        reduction.drain()


def scratch(groups, across):
    tiles = lambda *shape: pltpu.VMEM((*shape, 8, 128), F32)
    return [
        tiles(groups, across), tiles(groups // 2, across), tiles(groups // 2, across), tiles(3, groups // 8, across),
        tiles(groups // 8, across), tiles(7), tiles(), tiles(4), tiles(groups, across),
        pltpu.SemaphoreType.DMA((28,)), pltpu.SemaphoreType.DMA((28,)),
    ]


def main_part(panel, trailing):
    inner = pl.BlockSpec(memory_space=pltpu.VMEM)
    halves = pltpu.VMEM((32, 2, 8, 128), F32)
    return pl.pallas_call(
        main_kernel,
        out_shape=(
            jax.ShapeDtypeStruct((2048, 256), jnp.bfloat16),
            jax.ShapeDtypeStruct((2048, 256), jnp.bfloat16),
            jax.ShapeDtypeStruct((256, 256), F32),
            jax.ShapeDtypeStruct((256, 512), F32),
            jax.ShapeDtypeStruct((256, 512), jnp.bfloat16),
            jax.ShapeDtypeStruct((256, 512), jnp.bfloat16),
        ),
        in_specs=[pl.BlockSpec(memory_space=pltpu.HBM)] * 2,
        out_specs=(inner,) * 6,
        scratch_shapes=[
            pltpu.VMEM((4, 512, 256), F32),
            pltpu.VMEM((2048, 512), F32),
            halves,
            halves,
            halves,
            pltpu.SemaphoreType.DMA((2,)),
            pltpu.SemaphoreType.DMA((12,)),
            pltpu.SemaphoreType.DMA((12,)),
            *scratch(32, 2),
            *scratch(16, 4),
            *scratch(16, 4),
        ],
        compiler_params=pltpu.CompilerParams(collective_id=0, has_side_effects=True, vmem_limit_bytes=50 << 20),
    )(panel, trailing)


def update_kernel(trailing, high, low, weight_high, weight_low, rfactor, projected, rfactor_out, projected_out, updated):
    @pl.when(pl.program_id(0) == 0)
    def _():
        rfactor_out[...] = rfactor[...]
        projected_out[...] = projected[...]

    mul = functools.partial(jnp.dot, preferred_element_type=F32)
    x = high[...]
    updated[...] = trailing[...] - (mul(x, weight_high[...]) + (mul(x, weight_low[...]) + mul(low[...], weight_high[...])))


def update(trailing, high, low, weight_high, weight_low, rfactor, projected):
    rows = 256
    tile = pl.BlockSpec((rows, 512), lambda i: (i, 0))
    part = pl.BlockSpec((rows, 256), lambda i: (i, 0))
    fixed = pl.BlockSpec((256, 512), lambda i: (0, 0))
    square = pl.BlockSpec((256, 256), lambda i: (0, 0))
    return pl.pallas_call(
        update_kernel,
        grid=(2048 // rows,),
        out_shape=(
            jax.ShapeDtypeStruct((256, 256), F32),
            jax.ShapeDtypeStruct((256, 512), F32),
            jax.ShapeDtypeStruct((2048, 512), F32),
        ),
        in_specs=[tile, part, part, fixed, fixed, square, fixed],
        out_specs=(square, fixed, tile),
        compiler_params=pltpu.CompilerParams(vmem_limit_bytes=24 << 20),
    )(trailing, high, low, weight_high, weight_low, rfactor, projected)


def shards(panel, trailing):
    high, low, rfactor, projected, weight_high, weight_low = main_part(pltpu.with_memory_space_constraint(panel, pltpu.HBM), trailing)
    return update(trailing, high, low, weight_high, weight_low, rfactor, projected)


def solution(mesh):
    return jax.shard_map(
        shards,
        mesh=mesh,
        in_specs=(P(("rows", "cols"), None), P("rows", "cols")),
        out_specs=(P(), P(None, "cols"), P("rows", "cols")),
        check_vma=False,
    )
```

```python
import functools

import jax
import jax.numpy as jnp
from jax import lax
from jax.experimental import pallas as pl
from jax.experimental.pallas import tpu as pltpu
from jax.sharding import PartitionSpec as P

MESH = pl.DeviceIdType.MESH
HIGHEST = lax.Precision.HIGHEST
F32 = jnp.float32


def dot(left, right):
    return jnp.dot(left, right, precision=HIGHEST, preferred_element_type=F32)


class Place:
    def __init__(self):
        rows = lax.axis_index("rows")
        self.x = lax.axis_index("cols")
        self.core = lax.rem(rows, 2)
        self.z = lax.rem(rows // 2, 8)
        self.y = rows // 16

    def at(self, y=0, z=0, core=0, x=0):
        there = lax.rem(self.y + y, 4) * 16 + lax.rem(self.z + z, 8) * 2 + lax.rem(self.core + core, 2)
        return (there, lax.rem(self.x + x, 4))


def send(src, dst, send_sem, recv_sem, device):
    copy = pltpu.make_async_remote_copy(
        src_ref=src, dst_ref=dst, send_sem=send_sem, recv_sem=recv_sem, device_id=device, device_id_type=MESH
    )
    copy.start()
    return copy


PLANE = sorted(
    [(y, z) for y in range(4) for z in range(8) if (y, z) != (0, 0)], key=lambda d: (-min(d[0], 4 - d[0]) - min(d[1], 8 - d[1]), d)
)


class Reduction:
    def __init__(self, place, refs, over_x):
        self.place, self.over_x = place, over_x
        self.part, self.from_core, self.s1, self.from_y, self.s2, self.from_z, self.from_plane, self.s3, self.from_x, self.full = refs[:10]
        self.send_sem, self.recv_sem = refs[10:]
        self.groups, self.across = self.part.shape[:2]
        self.half, self.eighth = self.groups // 2, self.groups // 8
        self.copies = []

    def send(self, src, dst, device):
        used = len(self.copies)
        copy = send(src, dst, self.send_sem.at[used], self.recv_sem.at[used], device)
        self.copies.append(copy)
        return copy

    def start_core(self):
        p = self.place
        self.c1 = self.send(self.part.at[pl.ds(self.half * (1 - p.core), self.half)], self.from_core, p.at(core=1))

    def start_y(self):
        p, n = self.place, self.eighth
        self.c1.wait_recv()
        self.s1[...] = self.part[pl.ds(self.half * p.core, self.half)] + self.from_core[...]
        self.c2 = [self.send(self.s1.at[pl.ds(n * lax.rem(p.y + d, 4), n)], self.from_y.at[d - 1], p.at(y=d)) for d in (2, 1, 3)]

    def tile(self, y, z):
        return self.eighth * y + z // self.across, lax.rem(z, self.across)

    def start_plane(self):
        p = self.place
        self.c1.wait_recv()
        self.s1[...] = self.part[pl.ds(self.half * p.core, self.half)] + self.from_core[...]
        self.c3 = []
        for n, (y, z) in enumerate(PLANE):
            there = self.tile(lax.rem(p.y + y, 4), lax.rem(p.z + z, 8))
            self.c3.append(self.send(self.s1.at[there], self.from_plane.at[n], p.at(y=y, z=z)))

    def end_plane(self):
        terms = [self.s1[self.tile(self.place.y, self.place.z)]]
        for n in reversed(range(len(PLANE))):
            self.c3[n].wait_recv()
            terms.append(self.from_plane[n])
        while len(terms) > 1:
            terms = [a + b for a, b in zip(terms[::2], terms[1::2])]
        return terms[0]

    def start_z(self):
        p, n = self.place, self.eighth
        for c in self.c2:
            c.wait_recv()
        self.s2[...] = (self.s1[pl.ds(n * p.y, n)] + self.from_y[0]) + (self.from_y[1] + self.from_y[2])
        self.c3 = []
        for d in (4, 3, 5, 2, 6, 1, 7):
            there = lax.rem(p.z + d, 8)
            self.c3.append(self.send(self.s2.at[there // self.across, lax.rem(there, self.across)], self.from_z.at[d - 1], p.at(z=d)))

    def end_z(self):
        p = self.place
        for c in self.c3:
            c.wait_recv()
        f = self.from_z
        total = self.s2[p.z // self.across, lax.rem(p.z, self.across)]
        return ((total + f[0]) + (f[1] + f[2])) + ((f[3] + f[4]) + (f[5] + f[6]))

    def start_x(self):
        p = self.place
        self.s3[...] = self.end_z()
        self.c4 = [self.send(self.s3, self.from_x.at[p.x], p.at(x=d)) for d in (2, 1, 3)]
        self.from_x[p.x] = self.s3[...]

    def start_gather(self):
        p = self.place
        group, across = self.tile(p.y, p.z)
        group = self.half * p.core + group
        if self.over_x:
            for c in self.c4:
                c.wait_recv()
            self.full[group, across] = (self.from_x[0] + self.from_x[1]) + (self.from_x[2] + self.from_x[3])
        else:
            self.full[group, across] = self.end_plane()
        mine = self.full.at[group, across]
        self.c5 = [self.send(mine, mine, p.at(y=y, z=z)) for y, z in PLANE]

    def start_gather_core(self):
        p = self.place
        self.c7 = []
        for step in (0, 1, 3, 2):
            for c, (y, z) in zip(self.c5, PLANE):
                if y == (4 - step) % 4:
                    c.wait_recv()
            rows = self.full.at[pl.ds(self.half * p.core + self.eighth * lax.rem(p.y + step, 4), self.eighth)]
            self.c7.append(self.send(rows, rows, p.at(core=1)))

    def finish(self):
        for c in self.c7:
            c.wait_recv()

    def drain(self):
        for c in self.copies:
            c.wait_send()


def tiled(matrix):
    n = matrix.shape[0] // 8
    return [matrix[:, 128 * h : 128 * h + 128].reshape(n, 8, 128) for h in range(matrix.shape[1] // 128)]


def whole(ref):
    n, m = ref.shape[:2]
    return jnp.concatenate([ref[:, h].reshape(8 * n, 128) for h in range(m)], axis=1)


def row_of(x, j):
    return jnp.broadcast_to(x[j : j + 1, :], x.shape)


def lane_of(x, at):
    return jnp.take_along_axis(x, at, axis=1)


def eight_pivots(k, base, a, r, inv):
    sub = lax.broadcasted_iota(jnp.int32, (8, 128), 0)
    lane = lax.broadcasted_iota(jnp.int32, (8, 128), 1)
    rel = [lane + (128 * h - 8 * k) for h in range(2)]
    inside = [(x >= 0) & (x < 8) for x in rel]
    c = k // 16
    start = 8 * lax.rem(k, 16)
    ats = [jnp.zeros((8, 128), jnp.int32) + (start + j) for j in range(8)]
    d = a[k, c]
    cols = [lane_of(d, at) for at in ats]
    work = [jnp.where(inside[h], (rel[h] == sub).astype(F32), a[k, h]) for h in range(2)] + [d]
    outs = [jnp.zeros((8, 128), F32) for _ in work]
    for j in range(8):
        here = sub == j
        root = lax.rsqrt(row_of(cols[j], j))
        scaled = cols[j] * root
        for m in range(j + 1, 8):
            term = row_of(cols[m], j) * root
            cols[m] = jnp.where(here, term * root, cols[m] - scaled * term)
        for w in range(3):
            term = row_of(work[w], j) * root
            outs[w] = jnp.where(here, term, outs[w])
            rest = work[w] - scaled * term
            work[w] = rest if w == 2 else jnp.where(here, term * root, rest)
    for h in range(2):
        r[k, h] = jnp.where(rel[h] >= 8, outs[h], jnp.where(inside[h] & (rel[h] >= sub), outs[2], 0.0))
        inv[k, h] = jnp.where(rel[h] <= sub, outs[h], 0.0)
    rows = [[row_of(work[h], j) for j in range(8)] for h in range(2)]
    source = [a[base + g, c] for g in range(8)]
    new = [[jnp.where(inside[h], 0.0, a[base + g, h]) for h in range(2)] for g in range(8)]
    for j in range(8):
        for g in range(8):
            multiplier = lane_of(source[g], ats[j])
            for h in range(2):
                new[g][h] = new[g][h] - multiplier * rows[h][j]
    for g in range(8):
        for h in range(2):
            a[base + g, h] = new[g][h]


def take_out(s, a, r, inv):
    base = 8 * s
    rows = lambda ref, h: ref[pl.ds(base, 8), h].reshape(64, 128)
    right = []
    for h in range(2):
        col = lax.broadcasted_iota(jnp.int32, (64, 128), 1) + 128 * h
        right.append(jnp.where(col < 64 * (s + 1), rows(inv, h), rows(r, h)))
    right = jnp.concatenate(right, axis=1)
    for half in range((s + 1) // 2, 2):
        product = tiled(dot(rows(r, half).T, right))
        for h in range(2):
            col = lax.broadcasted_iota(jnp.int32, (16, 8, 128), 2) + 128 * h
            old = a[pl.ds(16 * half, 16), h]
            a[pl.ds(16 * half, 16), h] = jnp.where((col >= 64 * s) & (col < 64 * (s + 1)), 0.0, old) - product[h]


def factor_part(eighth, a, r, inv):
    s = eighth // 2

    def step(i, carry):
        eight_pivots(4 * eighth + i, 8 * s, a, r, inv)
        return carry

    lax.fori_loop(0, 4, step, 0)
    if eighth % 2 and s < 3:
        take_out(s, a, r, inv)


def split(x):
    high = x.astype(jnp.bfloat16)
    return high, (x - high.astype(F32)).astype(jnp.bfloat16)


def main_kernel(
    panel, trailing, block_high, block_low, rfactor, projected, weight_high, weight_low, held,
    block, a, inv, r, load_sem, side_send, side_recv, *rest
):
    p = Place()
    g = Reduction(p, rest[:12], True)
    t = [Reduction(p, rest[12 + 12 * q : 24 + 12 * q], False) for q in range(2)]

    owns = [
        pltpu.make_async_copy(panel.at[:, pl.ds(128 * q, 128)], block.at[p.x, q], load_sem.at[q]) for q in range(2)
    ]
    for own in owns:
        own.start()
    load = pltpu.make_async_copy(trailing, held, load_sem.at[2])

    barrier = pltpu.get_barrier_semaphore()
    peers = [p.at(core=1)] + [p.at(y=d) for d in (1, 2, 3)] + [p.at(z=d) for d in range(1, 8)] + [p.at(x=d) for d in (1, 2, 3)]
    for peer in peers:
        pl.semaphore_signal(barrier, inc=1, device_id=peer, device_id_type=MESH)
    pl.semaphore_wait(barrier, len(peers))
    for own in owns:
        own.wait()
    load.start()

    steps = (1, 3)
    x_copies = []

    def side_copy(source, q, half, side, slot):
        rows = block.at[source, q, pl.ds(256 * half, 256)]
        at = 6 * q + 2 * slot + side
        copy = send(rows, rows, side_send.at[at], side_recv.at[at], p.at(x=steps[side]))
        x_copies.append(copy)
        return copy

    def direct(q, n):
        return [side_copy(p.x, q, n if side == 0 else 1 - n, side, n) for side in range(2)]

    def relay(q, arrived):
        copies = []
        for side in range(2):
            arrived[side].wait_recv()
            copies.append(side_copy(lax.rem(p.x + steps[1 - side], 4), q, side, side, 2))
        return copies

    def wait(copies):
        for copy in copies:
            copy.wait_recv()

    def add_cross(q, step, first=False):
        x = lax.rem(p.x + step, 4)
        terms = tiled(dot(block[x, q].T, held[pl.ds(512 * x, 512), :]))
        for h in range(4):
            t[q].part[:, h] = terms[h] if first else t[q].part[:, h] + terms[h]

    first0 = direct(0, 0)
    second0 = direct(0, 1)
    mine = jnp.concatenate([block[p.x, q] for q in range(2)], axis=1)
    for h, tile in enumerate(tiled(dot(mine.T, mine))):
        g.part[:, h] = tile
    g.start_core()
    load.wait()
    add_cross(0, 0, True)
    g.start_y()
    relay0 = relay(0, first0)
    first1 = direct(1, 0)
    add_cross(1, 0, True)
    g.start_z()
    wait(second0)
    add_cross(0, 1)
    add_cross(0, 3)
    g.start_x()
    second1 = direct(1, 1)
    wait(relay0)
    add_cross(0, 2)
    t[0].start_core()
    relay1 = relay(1, first1)
    t[0].start_plane()
    g.start_gather()
    wait(second1)
    add_cross(1, 1)
    add_cross(1, 3)
    wait(relay1)
    add_cross(1, 2)
    t[1].start_core()
    g.start_gather_core()
    t[1].start_plane()
    t[0].start_gather()
    g.finish()
    a[...] = g.full[...]
    factor_part(0, a, r, inv)
    factor_part(1, a, r, inv)
    factor_part(2, a, r, inv)
    t[1].start_gather()
    factor_part(3, a, r, inv)
    t[0].start_gather_core()
    for x in range(4):
        for q in range(2):
            at = (pl.ds(512 * x, 512), pl.ds(128 * q, 128))
            block_high[at], block_low[at] = split(block[x, q])
    factor_part(4, a, r, inv)
    factor_part(5, a, r, inv)
    factor_part(6, a, r, inv)
    factor_part(7, a, r, inv)
    rfactor[...] = whole(r)
    inverse = whole(inv)
    square = dot(inverse.T, inverse)
    t[0].finish()
    upper = whole(t[0].full)
    projected[...] = dot(inverse[:, :128], upper)
    weight = dot(square[:, :128], upper)
    t[1].start_gather_core()
    t[1].finish()
    lower = whole(t[1].full)
    weight_high[...], weight_low[...] = split(weight + dot(square[:, 128:], lower))
    projected[128:, :] = projected[128:, :] + dot(inverse[128:, 128:], lower)
    for copy in x_copies:
        copy.wait_send()
    for reduction in (g, *t):
        reduction.drain()


def scratch(groups, across):
    tiles = lambda *shape: pltpu.VMEM((*shape, 8, 128), F32)
    return [
        tiles(groups, across), tiles(groups // 2, across), tiles(groups // 2, across), tiles(3, groups // 8, across),
        tiles(groups // 8, across), tiles(7), tiles(len(PLANE)), tiles(), tiles(4), tiles(groups, across),
        pltpu.SemaphoreType.DMA((72,)), pltpu.SemaphoreType.DMA((72,)),
    ]


def main_part(panel, trailing):
    inner = pl.BlockSpec(memory_space=pltpu.VMEM)
    halves = pltpu.VMEM((32, 2, 8, 128), F32)
    return pl.pallas_call(
        main_kernel,
        out_shape=(
            jax.ShapeDtypeStruct((2048, 256), jnp.bfloat16),
            jax.ShapeDtypeStruct((2048, 256), jnp.bfloat16),
            jax.ShapeDtypeStruct((256, 256), F32),
            jax.ShapeDtypeStruct((256, 512), F32),
            jax.ShapeDtypeStruct((256, 512), jnp.bfloat16),
            jax.ShapeDtypeStruct((256, 512), jnp.bfloat16),
            jax.ShapeDtypeStruct((2048, 512), F32),
        ),
        in_specs=[pl.BlockSpec(memory_space=pltpu.HBM)] * 2,
        out_specs=(inner,) * 7,
        scratch_shapes=[
            pltpu.VMEM((4, 2, 512, 128), F32),
            halves,
            halves,
            halves,
            pltpu.SemaphoreType.DMA((3,)),
            pltpu.SemaphoreType.DMA((12,)),
            pltpu.SemaphoreType.DMA((12,)),
            *scratch(32, 2),
            *scratch(16, 4),
            *scratch(16, 4),
        ],
        compiler_params=pltpu.CompilerParams(collective_id=0, has_side_effects=True, vmem_limit_bytes=40 << 20),
    )(panel, trailing)


ROWS = 256


def update_kernel(held, high, low, weight_high, weight_low, rfactor, projected, rfactor_out, projected_out, updated, tiles, sems):
    n = 2048 // ROWS
    copies = [
        pltpu.make_async_copy(rfactor, rfactor_out, sems.at[n]),
        pltpu.make_async_copy(projected, projected_out, sems.at[n + 1]),
    ]
    for copy in copies:
        copy.start()
    mul = functools.partial(jnp.dot, preferred_element_type=F32)
    for i in range(n):
        rows = pl.ds(ROWS * i, ROWS)
        x = high[rows, :]
        product = mul(x, weight_high[...]) + (mul(x, weight_low[...]) + mul(low[rows, :], weight_high[...]))
        tiles[i] = held[rows, :] - product
        copy = pltpu.make_async_copy(tiles.at[i], updated.at[rows], sems.at[i])
        copy.start()
        copies.append(copy)
    for copy in copies:
        copy.wait()


def update(*operands):
    inner, outer = pl.BlockSpec(memory_space=pltpu.VMEM), pl.BlockSpec(memory_space=pltpu.HBM)
    return pl.pallas_call(
        update_kernel,
        out_shape=(
            jax.ShapeDtypeStruct((256, 256), F32),
            jax.ShapeDtypeStruct((256, 512), F32),
            jax.ShapeDtypeStruct((2048, 512), F32),
        ),
        in_specs=[inner] * 7,
        out_specs=(outer,) * 3,
        scratch_shapes=[pltpu.VMEM((2048 // ROWS, ROWS, 512), F32), pltpu.SemaphoreType.DMA((2048 // ROWS + 2,))],
        compiler_params=pltpu.CompilerParams(vmem_limit_bytes=24 << 20),
    )(*operands)


def shards(panel, trailing):
    outside = [pltpu.with_memory_space_constraint(x, pltpu.HBM) for x in (panel, trailing)]
    high, low, rfactor, projected, weight_high, weight_low, held = main_part(*outside)
    return update(held, high, low, weight_high, weight_low, rfactor, projected)


def solution(mesh):
    return jax.shard_map(
        shards,
        mesh=mesh,
        in_specs=(P(("rows", "cols"), None), P("rows", "cols")),
        out_specs=(P(), P(None, "cols"), P("rows", "cols")),
        check_vma=False,
    )
```

```python
import functools

import jax
import jax.numpy as jnp
from jax import lax
from jax.experimental import pallas as pl
from jax.experimental.pallas import tpu as pltpu
from jax.sharding import PartitionSpec as P

MESH = pl.DeviceIdType.MESH
HIGHEST = lax.Precision.HIGHEST
F32 = jnp.float32


def dot(left, right):
    return jnp.dot(left, right, precision=HIGHEST, preferred_element_type=F32)


class Place:
    def __init__(self):
        rows = lax.axis_index("rows")
        self.x = lax.axis_index("cols")
        self.core = lax.rem(rows, 2)
        self.z = lax.rem(rows // 2, 8)
        self.y = rows // 16

    def at(self, y=0, z=0, core=0, x=0):
        there = lax.rem(self.y + y, 4) * 16 + lax.rem(self.z + z, 8) * 2 + lax.rem(self.core + core, 2)
        return (there, lax.rem(self.x + x, 4))


def send(src, dst, send_sem, recv_sem, device):
    copy = pltpu.make_async_remote_copy(
        src_ref=src, dst_ref=dst, send_sem=send_sem, recv_sem=recv_sem, device_id=device, device_id_type=MESH
    )
    copy.start()
    return copy


PLANE = sorted(
    [(y, z) for y in range(4) for z in range(8) if (y, z) != (0, 0)], key=lambda d: (-min(d[0], 4 - d[0]) - min(d[1], 8 - d[1]), d)
)


class Reduction:
    def __init__(self, place, refs, over_x):
        self.place, self.over_x = place, over_x
        self.part, self.from_core, self.s1, self.from_y, self.s2, self.from_z, self.from_plane, self.s3, self.from_x, self.full = refs[:10]
        self.send_sem, self.recv_sem = refs[10:]
        self.groups, self.across = self.part.shape[:2]
        self.half, self.eighth = self.groups // 2, self.groups // 8
        self.sent = []

    def send(self, src, dst, to, here, device):
        send(src, dst, self.send_sem.at[here], self.recv_sem.at[to], device)

    def all_sent(self, like, here):
        self.sent.append((like, here))

    def arrived(self, like, to):
        pltpu.make_async_copy(like, like, self.recv_sem.at[to]).wait()

    def start_core(self):
        p = self.place
        self.send(self.part.at[pl.ds(self.half * (1 - p.core), self.half)], self.from_core, 0, 0, p.at(core=1))
        self.all_sent(self.from_core, 0)

    def add_core(self):
        self.arrived(self.from_core, 0)
        self.s1[...] = self.part[pl.ds(self.half * self.place.core, self.half)] + self.from_core[...]

    def start_y(self):
        p, n = self.place, self.eighth
        self.add_core()
        for d in (2, 1, 3):
            self.send(self.s1.at[pl.ds(n * lax.rem(p.y + d, 4), n)], self.from_y.at[d - 1], 6, 3, p.at(y=d))
        self.all_sent(self.from_y, 3)

    def tile(self, y, z):
        return self.eighth * y + z // self.across, lax.rem(z, self.across)

    def start_plane(self):
        p = self.place
        self.add_core()
        for n, (y, z) in enumerate(PLANE):
            there = self.tile(lax.rem(p.y + y, 4), lax.rem(p.z + z, 8))
            self.send(self.s1.at[there], self.from_plane.at[n], 6, 3, p.at(y=y, z=z))
        self.all_sent(self.from_plane, 3)

    def end_plane(self):
        self.arrived(self.from_plane, 6)
        terms = [self.s1[self.tile(self.place.y, self.place.z)]] + [self.from_plane[n] for n in range(len(PLANE))]
        while len(terms) > 1:
            terms = [a + b for a, b in zip(terms[::2], terms[1::2])]
        return terms[0]

    def start_z(self):
        p, n = self.place, self.eighth
        self.arrived(self.from_y, 6)
        self.s2[...] = (self.s1[pl.ds(n * p.y, n)] + self.from_y[0]) + (self.from_y[1] + self.from_y[2])
        for d in (4, 3, 5, 2, 6, 1, 7):
            there = lax.rem(p.z + d, 8)
            self.send(self.s2.at[there // self.across, lax.rem(there, self.across)], self.from_z.at[d - 1], 7, 4, p.at(z=d))
        self.all_sent(self.from_z, 4)

    def end_z(self):
        p = self.place
        self.arrived(self.from_z, 7)
        f = self.from_z
        total = self.s2[p.z // self.across, lax.rem(p.z, self.across)]
        return ((total + f[0]) + (f[1] + f[2])) + ((f[3] + f[4]) + (f[5] + f[6]))

    def start_x(self):
        p = self.place
        self.s3[...] = self.end_z()
        for d in (2, 1, 3):
            self.send(self.s3, self.from_x.at[p.x], 8, 5, p.at(x=d))
        self.all_sent(self.from_x.at[pl.ds(0, 3)], 5)
        self.from_x[p.x] = self.s3[...]

    def start_gather(self):
        p = self.place
        group, across = self.tile(p.y, p.z)
        group = self.half * p.core + group
        if self.over_x:
            self.arrived(self.from_x.at[pl.ds(0, 3)], 8)
            self.full[group, across] = (self.from_x[0] + self.from_x[1]) + (self.from_x[2] + self.from_x[3])
        else:
            self.full[group, across] = self.end_plane()
        mine = self.full.at[group, across]
        for y, z in PLANE:
            self.send(mine, mine, 1 + y, 1, p.at(y=y, z=z))
        self.all_sent(self.from_plane, 1)

    def start_gather_core(self):
        p = self.place
        for step in (0, 1, 3, 2):
            rows = self.full.at[pl.ds(self.half * p.core + self.eighth * lax.rem(p.y + step, 4), self.eighth)]
            self.arrived(rows if step else self.from_z, 1 + (4 - step) % 4)
            self.send(rows, rows, 5, 2, p.at(core=1))
        self.all_sent(self.from_core, 2)

    def finish(self):
        self.arrived(self.from_core, 5)

    def drain(self):
        for like, here in self.sent:
            pltpu.make_async_copy(like, like, self.send_sem.at[here]).wait()


def tiled(matrix):
    n = matrix.shape[0] // 8
    return [matrix[:, 128 * h : 128 * h + 128].reshape(n, 8, 128) for h in range(matrix.shape[1] // 128)]


def whole(ref):
    n, m = ref.shape[:2]
    return jnp.concatenate([ref[:, h].reshape(8 * n, 128) for h in range(m)], axis=1)


def row_of(x, j):
    return jnp.broadcast_to(x[j : j + 1, :], x.shape)


def lane_of(x, at):
    return jnp.take_along_axis(x, at, axis=1)


def eight_pivots(k, base, a, r, inv):
    sub = lax.broadcasted_iota(jnp.int32, (8, 128), 0)
    lane = lax.broadcasted_iota(jnp.int32, (8, 128), 1)
    rel = [lane + (128 * h - 8 * k) for h in range(2)]
    inside = [(x >= 0) & (x < 8) for x in rel]
    c = k // 16
    start = 8 * lax.rem(k, 16)
    ats = [jnp.zeros((8, 128), jnp.int32) + (start + j) for j in range(8)]
    d = a[k, c]
    cols = [lane_of(d, at) for at in ats]
    work = [jnp.where(inside[h], (rel[h] == sub).astype(F32), a[k, h]) for h in range(2)] + [d]
    outs = [jnp.zeros((8, 128), F32) for _ in work]
    for j in range(8):
        here = sub == j
        root = lax.rsqrt(row_of(cols[j], j))
        scaled = cols[j] * root
        for m in range(j + 1, 8):
            term = row_of(cols[m], j) * root
            cols[m] = jnp.where(here, term * root, cols[m] - scaled * term)
        for w in range(3):
            term = row_of(work[w], j) * root
            outs[w] = jnp.where(here, term, outs[w])
            rest = work[w] - scaled * term
            work[w] = rest if w == 2 else jnp.where(here, term * root, rest)
    for h in range(2):
        r[k, h] = jnp.where(rel[h] >= 8, outs[h], jnp.where(inside[h] & (rel[h] >= sub), outs[2], 0.0))
        inv[k, h] = jnp.where(rel[h] <= sub, outs[h], 0.0)
    rows = [[row_of(work[h], j) for j in range(8)] for h in range(2)]
    source = [a[base + g, c] for g in range(8)]
    new = [[jnp.where(inside[h], 0.0, a[base + g, h]) for h in range(2)] for g in range(8)]
    for j in range(8):
        for g in range(8):
            multiplier = lane_of(source[g], ats[j])
            for h in range(2):
                new[g][h] = new[g][h] - multiplier * rows[h][j]
    for g in range(8):
        for h in range(2):
            a[base + g, h] = new[g][h]


def take_out(s, a, r, inv):
    base = 8 * s
    rows = lambda ref, h: ref[pl.ds(base, 8), h].reshape(64, 128)
    right = []
    for h in range(2):
        col = lax.broadcasted_iota(jnp.int32, (64, 128), 1) + 128 * h
        right.append(jnp.where(col < 64 * (s + 1), rows(inv, h), rows(r, h)))
    right = jnp.concatenate(right, axis=1)
    for half in range((s + 1) // 2, 2):
        product = tiled(dot(rows(r, half).T, right))
        for h in range(2):
            col = lax.broadcasted_iota(jnp.int32, (16, 8, 128), 2) + 128 * h
            old = a[pl.ds(16 * half, 16), h]
            a[pl.ds(16 * half, 16), h] = jnp.where((col >= 64 * s) & (col < 64 * (s + 1)), 0.0, old) - product[h]


def factor_part(eighth, a, r, inv):
    s = eighth // 2

    def step(i, carry):
        eight_pivots(4 * eighth + i, 8 * s, a, r, inv)
        return carry

    lax.fori_loop(0, 4, step, 0)
    if eighth % 2 and s < 3:
        take_out(s, a, r, inv)


def split(x):
    high = x.astype(jnp.bfloat16)
    return high, (x - high.astype(F32)).astype(jnp.bfloat16)


def main_kernel(
    panel, trailing, block_high, block_low, rfactor, projected, weight_high, weight_low, held,
    block, a, inv, r, load_sem, side_send, side_recv, *rest
):
    p = Place()
    g = Reduction(p, rest[:12], True)
    t = [Reduction(p, rest[12 + 12 * q : 24 + 12 * q], False) for q in range(2)]

    owns = [
        pltpu.make_async_copy(panel.at[:, pl.ds(128 * q, 128)], block.at[p.x, q], load_sem.at[q]) for q in range(2)
    ]
    for own in owns:
        own.start()
    load = pltpu.make_async_copy(trailing, held, load_sem.at[2])

    barrier = pltpu.get_barrier_semaphore()
    peers = [p.at(core=1)] + [p.at(y=d) for d in (1, 2, 3)] + [p.at(z=d) for d in range(1, 8)] + [p.at(x=d) for d in (1, 2, 3)]
    for peer in peers:
        pl.semaphore_signal(barrier, inc=1, device_id=peer, device_id_type=MESH)
    pl.semaphore_wait(barrier, len(peers))
    for own in owns:
        own.wait()
    load.start()

    steps = (1, 3)
    x_copies = []

    def side_copy(source, q, start, count, side):
        rows = block.at[source, q, pl.ds(start, count)]
        at = len(x_copies)
        copy = send(rows, rows, side_send.at[0], side_recv.at[at], p.at(x=steps[side]))
        x_copies.append(copy)
        return copy

    def direct(q, n, start=0, count=256):
        return [side_copy(p.x, q, 256 * (n if side == 0 else 1 - n) + start, count, side) for side in range(2)]

    def relay(q, *arrived):
        copies = []
        for side in range(2):
            for pair in arrived:
                pair[side].wait_recv()
            copies.append(side_copy(lax.rem(p.x + steps[1 - side], 4), q, 256 * side, 256, side))
        return copies

    def wait(copies):
        for copy in copies:
            copy.wait_recv()

    def add_cross(q, step, first=False):
        x = lax.rem(p.x + step, 4)
        terms = tiled(dot(block[x, q].T, held[pl.ds(512 * x, 512), :]))
        for h in range(4):
            t[q].part[:, h] = terms[h] if first else t[q].part[:, h] + terms[h]

    first0 = direct(0, 0)
    second0 = direct(0, 1)
    mine = jnp.concatenate([block[p.x, q] for q in range(2)], axis=1)
    for h, tile in enumerate(tiled(dot(mine.T, mine))):
        g.part[:, h] = tile
    g.start_core()
    g.start_y()
    load.wait()
    add_cross(0, 0, True)
    relay0 = relay(0, first0)
    first1 = direct(1, 0, 0, 128)
    g.start_z()
    add_cross(1, 0, True)
    wait(second0)
    add_cross(0, 1)
    add_cross(0, 3)
    g.start_x()
    rest1 = direct(1, 0, 128, 128)
    second1 = direct(1, 1)
    wait(relay0)
    add_cross(0, 2)
    t[0].start_core()
    t[0].start_plane()
    g.start_gather()
    relay1 = relay(1, first1, rest1)
    wait(second1)
    add_cross(1, 1)
    add_cross(1, 3)
    t[0].start_gather()
    wait(relay1)
    add_cross(1, 2)
    t[1].start_core()
    g.start_gather_core()
    t[1].start_plane()
    g.finish()
    a[...] = g.full[...]
    factor_part(0, a, r, inv)
    factor_part(1, a, r, inv)
    factor_part(2, a, r, inv)
    factor_part(3, a, r, inv)
    t[0].start_gather_core()
    factor_part(4, a, r, inv)
    t[1].start_gather()
    for x in range(4):
        for q in range(2):
            at = (pl.ds(512 * x, 512), pl.ds(128 * q, 128))
            block_high[at], block_low[at] = split(block[x, q])
    factor_part(5, a, r, inv)
    factor_part(6, a, r, inv)
    factor_part(7, a, r, inv)
    rfactor[...] = whole(r)
    inverse = whole(inv)
    square = dot(inverse.T, inverse)
    t[0].finish()
    upper = whole(t[0].full)
    projected[...] = dot(inverse[:, :128], upper)
    weight = dot(square[:, :128], upper)
    t[1].start_gather_core()
    t[1].finish()
    lower = whole(t[1].full)
    weight_high[...], weight_low[...] = split(weight + dot(square[:, 128:], lower))
    projected[128:, :] = projected[128:, :] + dot(inverse[128:, 128:], lower)
    sent = block.at[pl.ds(0, 3)]
    pltpu.make_async_copy(sent, sent, side_send.at[0]).wait()
    for reduction in (g, *t):
        reduction.drain()


def scratch(groups, across):
    tiles = lambda *shape: pltpu.VMEM((*shape, 8, 128), F32)
    return [
        tiles(groups, across), tiles(groups // 2, across), tiles(groups // 2, across), tiles(3, groups // 8, across),
        tiles(groups // 8, across), tiles(7), tiles(len(PLANE)), tiles(), tiles(4), tiles(groups, across),
        pltpu.SemaphoreType.DMA((6,)), pltpu.SemaphoreType.DMA((9,)),
    ]


def main_part(panel, trailing):
    inner = pl.BlockSpec(memory_space=pltpu.VMEM)
    halves = pltpu.VMEM((32, 2, 8, 128), F32)
    return pl.pallas_call(
        main_kernel,
        out_shape=(
            jax.ShapeDtypeStruct((2048, 256), jnp.bfloat16),
            jax.ShapeDtypeStruct((2048, 256), jnp.bfloat16),
            jax.ShapeDtypeStruct((256, 256), F32),
            jax.ShapeDtypeStruct((256, 512), F32),
            jax.ShapeDtypeStruct((256, 512), jnp.bfloat16),
            jax.ShapeDtypeStruct((256, 512), jnp.bfloat16),
            jax.ShapeDtypeStruct((2048, 512), F32),
        ),
        in_specs=[pl.BlockSpec(memory_space=pltpu.HBM)] * 2,
        out_specs=(inner,) * 7,
        scratch_shapes=[
            pltpu.VMEM((4, 2, 512, 128), F32),
            halves,
            halves,
            halves,
            pltpu.SemaphoreType.DMA((3,)),
            pltpu.SemaphoreType.DMA((1,)),
            pltpu.SemaphoreType.DMA((14,)),
            *scratch(32, 2),
            *scratch(16, 4),
            *scratch(16, 4),
        ],
        compiler_params=pltpu.CompilerParams(collective_id=0, has_side_effects=True, vmem_limit_bytes=40 << 20),
    )(panel, trailing)


ROWS = 256


def update_kernel(held, high, low, weight_high, weight_low, rfactor, projected, rfactor_out, projected_out, updated, tiles, sems):
    n = 2048 // ROWS
    copies = [
        pltpu.make_async_copy(rfactor, rfactor_out, sems.at[n]),
        pltpu.make_async_copy(projected, projected_out, sems.at[n + 1]),
    ]
    for copy in copies:
        copy.start()
    mul = functools.partial(jnp.dot, preferred_element_type=F32)
    for i in range(n):
        rows = pl.ds(ROWS * i, ROWS)
        x = high[rows, :]
        product = mul(x, weight_high[...]) + (mul(x, weight_low[...]) + mul(low[rows, :], weight_high[...]))
        tiles[i] = held[rows, :] - product
        copy = pltpu.make_async_copy(tiles.at[i], updated.at[rows], sems.at[i])
        copy.start()
        copies.append(copy)
    for copy in copies:
        copy.wait()


def update(*operands):
    inner, outer = pl.BlockSpec(memory_space=pltpu.VMEM), pl.BlockSpec(memory_space=pltpu.HBM)
    return pl.pallas_call(
        update_kernel,
        out_shape=(
            jax.ShapeDtypeStruct((256, 256), F32),
            jax.ShapeDtypeStruct((256, 512), F32),
            jax.ShapeDtypeStruct((2048, 512), F32),
        ),
        in_specs=[inner] * 7,
        out_specs=(outer,) * 3,
        scratch_shapes=[pltpu.VMEM((2048 // ROWS, ROWS, 512), F32), pltpu.SemaphoreType.DMA((2048 // ROWS + 2,))],
        compiler_params=pltpu.CompilerParams(vmem_limit_bytes=24 << 20),
    )(*operands)


def shards(panel, trailing):
    outside = [pltpu.with_memory_space_constraint(x, pltpu.HBM) for x in (panel, trailing)]
    high, low, rfactor, projected, weight_high, weight_low, held = main_part(*outside)
    return update(held, high, low, weight_high, weight_low, rfactor, projected)


def solution(mesh):
    return jax.shard_map(
        shards,
        mesh=mesh,
        in_specs=(P(("rows", "cols"), None), P("rows", "cols")),
        out_specs=(P(), P(None, "cols"), P("rows", "cols")),
        check_vma=False,
    )
```

```python
import functools

import jax
import jax.numpy as jnp
from jax import lax
from jax.experimental import pallas as pl
from jax.experimental.pallas import tpu as pltpu
from jax.sharding import PartitionSpec as P

MESH = pl.DeviceIdType.MESH
HIGHEST = lax.Precision.HIGHEST
F32 = jnp.float32


def dot(left, right):
    return jnp.dot(left, right, precision=HIGHEST, preferred_element_type=F32)


class Place:
    def __init__(self):
        rows = lax.axis_index("rows")
        self.x = lax.axis_index("cols")
        self.core = lax.rem(rows, 2)
        self.z = lax.rem(rows // 2, 8)
        self.y = rows // 16

    def at(self, y=0, z=0, core=0, x=0):
        there = lax.rem(self.y + y, 4) * 16 + lax.rem(self.z + z, 8) * 2 + lax.rem(self.core + core, 2)
        return (there, lax.rem(self.x + x, 4))


def send(src, dst, send_sem, recv_sem, device):
    copy = pltpu.make_async_remote_copy(
        src_ref=src, dst_ref=dst, send_sem=send_sem, recv_sem=recv_sem, device_id=device, device_id_type=MESH
    )
    copy.start()
    return copy


PLANE = sorted(
    [(y, z) for y in range(4) for z in range(8) if (y, z) != (0, 0)], key=lambda d: (-min(d[0], 4 - d[0]) - min(d[1], 8 - d[1]), d)
)


class Reduction:
    def __init__(self, place, refs, over_x):
        self.place, self.over_x = place, over_x
        self.part, self.from_core, self.s1, self.from_y, self.s2, self.from_z, self.from_plane, self.s3, self.from_x, self.full = refs[:10]
        self.send_sem, self.recv_sem = refs[10:]
        self.groups, self.across = self.part.shape[:2]
        self.half, self.eighth = self.groups // 2, self.groups // 8
        self.sent = []

    def send(self, src, dst, to, here, device):
        send(src, dst, self.send_sem.at[here], self.recv_sem.at[to], device)

    def all_sent(self, like, here):
        self.sent.append((like, here))

    def arrived(self, like, to):
        pltpu.make_async_copy(like, like, self.recv_sem.at[to]).wait()

    def start_core(self):
        p = self.place
        self.send(self.part.at[pl.ds(self.half * (1 - p.core), self.half)], self.from_core, 0, 0, p.at(core=1))
        self.all_sent(self.from_core, 0)

    def add_core(self):
        self.arrived(self.from_core, 0)
        self.s1[...] = self.part[pl.ds(self.half * self.place.core, self.half)] + self.from_core[...]

    def start_y(self):
        p, n = self.place, self.eighth
        self.add_core()
        for d in (2, 1, 3):
            self.send(self.s1.at[pl.ds(n * lax.rem(p.y + d, 4), n)], self.from_y.at[d - 1], 6, 3, p.at(y=d))
        self.all_sent(self.from_y, 3)

    def tile(self, y, z):
        return self.eighth * y + z // self.across, lax.rem(z, self.across)

    def start_plane(self):
        p = self.place
        self.add_core()
        for n, (y, z) in enumerate(PLANE):
            there = self.tile(lax.rem(p.y + y, 4), lax.rem(p.z + z, 8))
            self.send(self.s1.at[there], self.from_plane.at[n], 6, 3, p.at(y=y, z=z))
        self.all_sent(self.from_plane, 3)

    def end_plane(self):
        self.arrived(self.from_plane, 6)
        terms = [self.s1[self.tile(self.place.y, self.place.z)]] + [self.from_plane[n] for n in range(len(PLANE))]
        while len(terms) > 1:
            terms = [a + b for a, b in zip(terms[::2], terms[1::2])]
        return terms[0]

    def start_z(self):
        p, n = self.place, self.eighth
        self.arrived(self.from_y, 6)
        self.s2[...] = (self.s1[pl.ds(n * p.y, n)] + self.from_y[0]) + (self.from_y[1] + self.from_y[2])
        for d in (4, 3, 5, 2, 6, 1, 7):
            there = lax.rem(p.z + d, 8)
            self.send(self.s2.at[there // self.across, lax.rem(there, self.across)], self.from_z.at[d - 1], 7, 4, p.at(z=d))
        self.all_sent(self.from_z, 4)

    def end_z(self):
        p = self.place
        self.arrived(self.from_z, 7)
        f = self.from_z
        total = self.s2[p.z // self.across, lax.rem(p.z, self.across)]
        return ((total + f[0]) + (f[1] + f[2])) + ((f[3] + f[4]) + (f[5] + f[6]))

    def start_x(self):
        p = self.place
        self.s3[...] = self.end_z()
        for d in (2, 1, 3):
            self.send(self.s3, self.from_x.at[p.x], 8, 5, p.at(x=d))
        self.all_sent(self.from_x.at[pl.ds(0, 3)], 5)
        self.from_x[p.x] = self.s3[...]

    def start_gather(self):
        p = self.place
        group, across = self.tile(p.y, p.z)
        group = self.half * p.core + group
        if self.over_x:
            self.arrived(self.from_x.at[pl.ds(0, 3)], 8)
            self.full[group, across] = (self.from_x[0] + self.from_x[1]) + (self.from_x[2] + self.from_x[3])
        else:
            self.full[group, across] = self.end_plane()
        mine = self.full.at[group, across]
        for y, z in PLANE:
            self.send(mine, mine, 1 + y, 1, p.at(y=y, z=z))
        self.all_sent(self.from_plane, 1)

    def start_gather_core(self):
        p = self.place
        for step in (0, 1, 3, 2):
            rows = self.full.at[pl.ds(self.half * p.core + self.eighth * lax.rem(p.y + step, 4), self.eighth)]
            self.arrived(rows if step else self.from_z, 1 + (4 - step) % 4)
            self.send(rows, rows, 5, 2, p.at(core=1))
        self.all_sent(self.from_core, 2)

    def finish(self):
        self.arrived(self.from_core, 5)

    def drain(self):
        for like, here in self.sent:
            pltpu.make_async_copy(like, like, self.send_sem.at[here]).wait()


def tiled(matrix):
    n = matrix.shape[0] // 8
    return [matrix[:, 128 * h : 128 * h + 128].reshape(n, 8, 128) for h in range(matrix.shape[1] // 128)]


def whole(ref):
    n, m = ref.shape[:2]
    return jnp.concatenate([ref[:, h].reshape(8 * n, 128) for h in range(m)], axis=1)


def row_of(x, j):
    return jnp.broadcast_to(x[j : j + 1, :], x.shape)


def lane_of(x, at):
    return jnp.take_along_axis(x, at, axis=1)


def eight_pivots(k, base, a, r, inv):
    sub = lax.broadcasted_iota(jnp.int32, (8, 128), 0)
    lane = lax.broadcasted_iota(jnp.int32, (8, 128), 1)
    rel = [lane + (128 * h - 8 * k) for h in range(2)]
    inside = [(x >= 0) & (x < 8) for x in rel]
    c = k // 16
    start = 8 * lax.rem(k, 16)
    ats = [jnp.zeros((8, 128), jnp.int32) + (start + j) for j in range(8)]
    d = a[k, c]
    cols = [lane_of(d, at) for at in ats]
    work = [jnp.where(inside[h], (rel[h] == sub).astype(F32), a[k, h]) for h in range(2)] + [d]
    outs = [jnp.zeros((8, 128), F32) for _ in work]
    for j in range(8):
        here = sub == j
        root = lax.rsqrt(row_of(cols[j], j))
        scaled = cols[j] * root
        for m in range(j + 1, 8):
            term = row_of(cols[m], j) * root
            cols[m] = jnp.where(here, term * root, cols[m] - scaled * term)
        for w in range(3):
            term = row_of(work[w], j) * root
            outs[w] = jnp.where(here, term, outs[w])
            rest = work[w] - scaled * term
            work[w] = rest if w == 2 else jnp.where(here, term * root, rest)
    for h in range(2):
        r[k, h] = jnp.where(rel[h] >= 8, outs[h], jnp.where(inside[h] & (rel[h] >= sub), outs[2], 0.0))
        inv[k, h] = jnp.where(rel[h] <= sub, outs[h], 0.0)
    rows = [[row_of(work[h], j) for j in range(8)] for h in range(2)]
    source = [a[base + g, c] for g in range(8)]
    new = [[jnp.where(inside[h], 0.0, a[base + g, h]) for h in range(2)] for g in range(8)]
    for j in range(8):
        for g in range(8):
            multiplier = lane_of(source[g], ats[j])
            for h in range(2):
                new[g][h] = new[g][h] - multiplier * rows[h][j]
    for g in range(8):
        for h in range(2):
            a[base + g, h] = new[g][h]


def take_out(s, a, r, inv):
    base = 8 * s
    rows = lambda ref, h: ref[pl.ds(base, 8), h].reshape(64, 128)
    right = []
    for h in range(2):
        col = lax.broadcasted_iota(jnp.int32, (64, 128), 1) + 128 * h
        right.append(jnp.where(col < 64 * (s + 1), rows(inv, h), rows(r, h)))
    right = jnp.concatenate(right, axis=1)
    for half in range((s + 1) // 2, 2):
        product = tiled(dot(rows(r, half).T, right))
        for h in range(2):
            col = lax.broadcasted_iota(jnp.int32, (16, 8, 128), 2) + 128 * h
            old = a[pl.ds(16 * half, 16), h]
            a[pl.ds(16 * half, 16), h] = jnp.where((col >= 64 * s) & (col < 64 * (s + 1)), 0.0, old) - product[h]


def factor_part(eighth, a, r, inv):
    s = eighth // 2

    def step(i, carry):
        eight_pivots(4 * eighth + i, 8 * s, a, r, inv)
        return carry

    lax.fori_loop(0, 4, step, 0)
    if eighth % 2 and s < 3:
        take_out(s, a, r, inv)


def split(x):
    high = x.astype(jnp.bfloat16)
    return high, (x - high.astype(F32)).astype(jnp.bfloat16)


def main_kernel(
    panel, trailing, block_high, block_low, rfactor, projected, weight_high, weight_low, held,
    block, a, inv, r, load_sem, side_send, side_recv, met, *rest
):
    p = Place()
    g = Reduction(p, rest[:12], True)
    t = [Reduction(p, rest[12 + 12 * q : 24 + 12 * q], False) for q in range(2)]

    owns = [
        pltpu.make_async_copy(panel.at[:, pl.ds(128 * q, 128)], block.at[p.x, q], load_sem.at[q]) for q in range(2)
    ]
    for own in owns:
        own.start()
    load = pltpu.make_async_copy(trailing, held, load_sem.at[2])

    beside = {axis: [p.at(**{axis: d}) for d in (1, size - 1)] for axis, size in (("y", 4), ("z", 8), ("x", 4))}
    barrier = pltpu.get_barrier_semaphore()
    for peer in [p.at(core=1)] + beside["y"] + beside["z"] + beside["x"]:
        pl.semaphore_signal(barrier, inc=1, device_id=peer, device_id_type=MESH)
    pl.semaphore_wait(barrier, 7)

    def tell(axis, at):
        for peer in beside[axis]:
            pl.semaphore_signal(met.at[at], inc=1, device_id=peer, device_id_type=MESH)

    def hear(at):
        pl.semaphore_wait(met.at[at], 2)

    for at, axis in enumerate(("y", "x", "z")):
        tell(axis, at)
    for own in owns:
        own.wait()
    load.start()

    steps = (1, 3)
    x_copies = []

    def side_copy(source, q, start, count, side):
        rows = block.at[source, q, pl.ds(start, count)]
        at = len(x_copies)
        copy = send(rows, rows, side_send.at[0], side_recv.at[at], p.at(x=steps[side]))
        x_copies.append(copy)
        return copy

    def direct(q, n, start=0, count=256):
        return [side_copy(p.x, q, 256 * (n if side == 0 else 1 - n) + start, count, side) for side in range(2)]

    def relay(q, *arrived):
        copies = []
        for side in range(2):
            for pair in arrived:
                pair[side].wait_recv()
            copies.append(side_copy(lax.rem(p.x + steps[1 - side], 4), q, 256 * side, 256, side))
        return copies

    def wait(copies):
        for copy in copies:
            copy.wait_recv()

    def add_cross(q, step, first=False):
        x = lax.rem(p.x + step, 4)
        terms = tiled(dot(block[x, q].T, held[pl.ds(512 * x, 512), :]))
        for h in range(4):
            t[q].part[:, h] = terms[h] if first else t[q].part[:, h] + terms[h]

    first0 = direct(0, 0)
    second0 = direct(0, 1)
    mine = jnp.concatenate([block[p.x, q] for q in range(2)], axis=1)
    for h, tile in enumerate(tiled(dot(mine.T, mine))):
        g.part[:, h] = tile
    g.start_core()
    hear(0)
    hear(2)
    tell("z", 3)
    g.start_y()
    hear(3)
    tell("z", 4)
    load.wait()
    add_cross(0, 0, True)
    relay0 = relay(0, first0)
    first1 = direct(1, 0, 0, 128)
    hear(4)
    hear(1)
    g.start_z()
    add_cross(1, 0, True)
    wait(second0)
    add_cross(0, 1)
    add_cross(0, 3)
    g.start_x()
    rest1 = direct(1, 0, 128, 128)
    second1 = direct(1, 1)
    wait(relay0)
    add_cross(0, 2)
    t[0].start_core()
    t[0].start_plane()
    g.start_gather()
    relay1 = relay(1, first1, rest1)
    wait(second1)
    add_cross(1, 1)
    add_cross(1, 3)
    t[0].start_gather()
    wait(relay1)
    add_cross(1, 2)
    t[1].start_core()
    g.start_gather_core()
    t[1].start_plane()
    g.finish()
    a[...] = g.full[...]
    factor_part(0, a, r, inv)
    factor_part(1, a, r, inv)
    factor_part(2, a, r, inv)
    factor_part(3, a, r, inv)
    t[0].start_gather_core()
    factor_part(4, a, r, inv)
    t[1].start_gather()
    for x in range(4):
        for q in range(2):
            at = (pl.ds(512 * x, 512), pl.ds(128 * q, 128))
            block_high[at], block_low[at] = split(block[x, q])
    factor_part(5, a, r, inv)
    factor_part(6, a, r, inv)
    factor_part(7, a, r, inv)
    rfactor[...] = whole(r)
    inverse = whole(inv)
    square = dot(inverse.T, inverse)
    t[0].finish()
    upper = whole(t[0].full)
    projected[...] = dot(inverse[:, :128], upper)
    weight = dot(square[:, :128], upper)
    t[1].start_gather_core()
    t[1].finish()
    lower = whole(t[1].full)
    weight_high[...], weight_low[...] = split(weight + dot(square[:, 128:], lower))
    projected[128:, :] = projected[128:, :] + dot(inverse[128:, 128:], lower)
    sent = block.at[pl.ds(0, 3)]
    pltpu.make_async_copy(sent, sent, side_send.at[0]).wait()
    for reduction in (g, *t):
        reduction.drain()


def scratch(groups, across):
    tiles = lambda *shape: pltpu.VMEM((*shape, 8, 128), F32)
    return [
        tiles(groups, across), tiles(groups // 2, across), tiles(groups // 2, across), tiles(3, groups // 8, across),
        tiles(groups // 8, across), tiles(7), tiles(len(PLANE)), tiles(), tiles(4), tiles(groups, across),
        pltpu.SemaphoreType.DMA((6,)), pltpu.SemaphoreType.DMA((9,)),
    ]


def main_part(panel, trailing):
    inner = pl.BlockSpec(memory_space=pltpu.VMEM)
    halves = pltpu.VMEM((32, 2, 8, 128), F32)
    return pl.pallas_call(
        main_kernel,
        out_shape=(
            jax.ShapeDtypeStruct((2048, 256), jnp.bfloat16),
            jax.ShapeDtypeStruct((2048, 256), jnp.bfloat16),
            jax.ShapeDtypeStruct((256, 256), F32),
            jax.ShapeDtypeStruct((256, 512), F32),
            jax.ShapeDtypeStruct((256, 512), jnp.bfloat16),
            jax.ShapeDtypeStruct((256, 512), jnp.bfloat16),
            jax.ShapeDtypeStruct((2048, 512), F32),
        ),
        in_specs=[pl.BlockSpec(memory_space=pltpu.HBM)] * 2,
        out_specs=(inner,) * 7,
        scratch_shapes=[
            pltpu.VMEM((4, 2, 512, 128), F32),
            halves,
            halves,
            halves,
            pltpu.SemaphoreType.DMA((3,)),
            pltpu.SemaphoreType.DMA((1,)),
            pltpu.SemaphoreType.DMA((14,)),
            pltpu.SemaphoreType.REGULAR((5,)),
            *scratch(32, 2),
            *scratch(16, 4),
            *scratch(16, 4),
        ],
        compiler_params=pltpu.CompilerParams(collective_id=0, has_side_effects=True, vmem_limit_bytes=40 << 20),
    )(panel, trailing)


ROWS = 256


def update_kernel(held, high, low, weight_high, weight_low, rfactor, projected, rfactor_out, projected_out, updated, tiles, sems):
    n = 2048 // ROWS
    copies = [
        pltpu.make_async_copy(rfactor, rfactor_out, sems.at[n]),
        pltpu.make_async_copy(projected, projected_out, sems.at[n + 1]),
    ]
    for copy in copies:
        copy.start()
    mul = functools.partial(jnp.dot, preferred_element_type=F32)
    for i in range(n):
        rows = pl.ds(ROWS * i, ROWS)
        x = high[rows, :]
        product = mul(x, weight_high[...]) + (mul(x, weight_low[...]) + mul(low[rows, :], weight_high[...]))
        tiles[i] = held[rows, :] - product
        copy = pltpu.make_async_copy(tiles.at[i], updated.at[rows], sems.at[i])
        copy.start()
        copies.append(copy)
    for copy in copies:
        copy.wait()


def update(*operands):
    inner, outer = pl.BlockSpec(memory_space=pltpu.VMEM), pl.BlockSpec(memory_space=pltpu.HBM)
    return pl.pallas_call(
        update_kernel,
        out_shape=(
            jax.ShapeDtypeStruct((256, 256), F32),
            jax.ShapeDtypeStruct((256, 512), F32),
            jax.ShapeDtypeStruct((2048, 512), F32),
        ),
        in_specs=[inner] * 7,
        out_specs=(outer,) * 3,
        scratch_shapes=[pltpu.VMEM((2048 // ROWS, ROWS, 512), F32), pltpu.SemaphoreType.DMA((2048 // ROWS + 2,))],
        compiler_params=pltpu.CompilerParams(vmem_limit_bytes=24 << 20),
    )(*operands)


def shards(panel, trailing):
    outside = [pltpu.with_memory_space_constraint(x, pltpu.HBM) for x in (panel, trailing)]
    high, low, rfactor, projected, weight_high, weight_low, held = main_part(*outside)
    return update(held, high, low, weight_high, weight_low, rfactor, projected)


def solution(mesh):
    return jax.shard_map(
        shards,
        mesh=mesh,
        in_specs=(P(("rows", "cols"), None), P("rows", "cols")),
        out_specs=(P(), P(None, "cols"), P("rows", "cols")),
        check_vma=False,
    )
```

```python
import functools

import jax
import jax.numpy as jnp
from jax import lax
from jax.experimental import pallas as pl
from jax.experimental.pallas import tpu as pltpu
from jax.sharding import PartitionSpec as P

MESH = pl.DeviceIdType.MESH
HIGHEST = lax.Precision.HIGHEST
F32 = jnp.float32


def dot(left, right):
    return jnp.dot(left, right, precision=HIGHEST, preferred_element_type=F32)


class Place:
    def __init__(self):
        rows = lax.axis_index("rows")
        self.x = lax.axis_index("cols")
        self.core = lax.rem(rows, 2)
        self.z = lax.rem(rows // 2, 8)
        self.y = rows // 16

    def at(self, y=0, z=0, core=0, x=0):
        there = lax.rem(self.y + y, 4) * 16 + lax.rem(self.z + z, 8) * 2 + lax.rem(self.core + core, 2)
        return (there, lax.rem(self.x + x, 4))


def send(src, dst, send_sem, recv_sem, device):
    copy = pltpu.make_async_remote_copy(
        src_ref=src, dst_ref=dst, send_sem=send_sem, recv_sem=recv_sem, device_id=device, device_id_type=MESH
    )
    copy.start()
    return copy


PLANE = sorted(
    [(y, z) for y in range(4) for z in range(8) if (y, z) != (0, 0)], key=lambda d: (-min(d[0], 4 - d[0]) - min(d[1], 8 - d[1]), d)
)


class Reduction:
    def __init__(self, place, refs, over_x):
        self.place, self.over_x = place, over_x
        self.part, self.from_core, self.s1, self.from_y, self.s2, self.from_z, self.from_plane, self.s3, self.from_x, self.full = refs[:10]
        self.send_sem, self.recv_sem = refs[10:]
        self.groups, self.across = self.part.shape[:2]
        self.half, self.eighth = self.groups // 2, self.groups // 8
        self.sent = []

    def send(self, src, dst, to, here, device):
        send(src, dst, self.send_sem.at[here], self.recv_sem.at[to], device)

    def all_sent(self, like, here):
        self.sent.append((like, here))

    def arrived(self, like, to):
        pltpu.make_async_copy(like, like, self.recv_sem.at[to]).wait()

    def start_core(self, column=0, columns=None):
        p, n = self.place, columns or self.across
        theirs = self.part.at[pl.ds(self.half * (1 - p.core), self.half), pl.ds(column, n)]
        self.send(theirs, self.from_core.at[:, pl.ds(column, n)], 0, 0, p.at(core=1))
        if column + n == self.across:
            self.all_sent(self.from_core, 0)

    def add_core(self):
        self.arrived(self.from_core, 0)
        self.s1[...] = self.part[pl.ds(self.half * self.place.core, self.half)] + self.from_core[...]

    def start_y(self):
        p, n = self.place, self.eighth
        self.add_core()
        for d in (2, 1, 3):
            self.send(self.s1.at[pl.ds(n * lax.rem(p.y + d, 4), n)], self.from_y.at[d - 1], 6, 3, p.at(y=d))
        self.all_sent(self.from_y, 3)

    def tile(self, y, z):
        return self.eighth * y + z // self.across, lax.rem(z, self.across)

    def start_plane(self):
        p = self.place
        self.add_core()
        for n, (y, z) in enumerate(PLANE):
            there = self.tile(lax.rem(p.y + y, 4), lax.rem(p.z + z, 8))
            self.send(self.s1.at[there], self.from_plane.at[n], 6, 3, p.at(y=y, z=z))
        self.all_sent(self.from_plane, 3)

    def end_plane(self):
        self.arrived(self.from_plane, 6)
        terms = [self.s1[self.tile(self.place.y, self.place.z)]] + [self.from_plane[n] for n in range(len(PLANE))]
        while len(terms) > 1:
            terms = [a + b for a, b in zip(terms[::2], terms[1::2])]
        return terms[0]

    def start_z(self):
        p, n = self.place, self.eighth
        self.arrived(self.from_y, 6)
        self.s2[...] = (self.s1[pl.ds(n * p.y, n)] + self.from_y[0]) + (self.from_y[1] + self.from_y[2])
        for d in (4, 3, 5, 2, 6, 1, 7):
            there = lax.rem(p.z + d, 8)
            self.send(self.s2.at[there // self.across, lax.rem(there, self.across)], self.from_z.at[d - 1], 7, 4, p.at(z=d))
        self.all_sent(self.from_z, 4)

    def end_z(self):
        p = self.place
        self.arrived(self.from_z, 7)
        f = self.from_z
        total = self.s2[p.z // self.across, lax.rem(p.z, self.across)]
        return ((total + f[0]) + (f[1] + f[2])) + ((f[3] + f[4]) + (f[5] + f[6]))

    def start_x(self):
        p = self.place
        self.s3[...] = self.end_z()
        for d in (2, 1, 3):
            self.send(self.s3, self.from_x.at[p.x], 8, 5, p.at(x=d))
        self.all_sent(self.from_x.at[pl.ds(0, 3)], 5)
        self.from_x[p.x] = self.s3[...]

    def start_gather(self):
        p = self.place
        group, across = self.tile(p.y, p.z)
        group = self.half * p.core + group
        if self.over_x:
            self.arrived(self.from_x.at[pl.ds(0, 3)], 8)
            self.full[group, across] = (self.from_x[0] + self.from_x[1]) + (self.from_x[2] + self.from_x[3])
        else:
            self.full[group, across] = self.end_plane()
        mine = self.full.at[group, across]
        for y, z in PLANE:
            self.send(mine, mine, 1 + y, 1, p.at(y=y, z=z))
        self.all_sent(self.from_plane, 1)

    def start_gather_core(self):
        p = self.place
        for step in (0, 1, 3, 2):
            rows = self.full.at[pl.ds(self.half * p.core + self.eighth * lax.rem(p.y + step, 4), self.eighth)]
            self.arrived(rows if step else self.from_z, 1 + (4 - step) % 4)
            self.send(rows, rows, 5, 2, p.at(core=1))
        self.all_sent(self.from_core, 2)

    def finish(self):
        self.arrived(self.from_core, 5)

    def drain(self):
        for like, here in self.sent:
            pltpu.make_async_copy(like, like, self.send_sem.at[here]).wait()


def tiled(matrix):
    n = matrix.shape[0] // 8
    return [matrix[:, 128 * h : 128 * h + 128].reshape(n, 8, 128) for h in range(matrix.shape[1] // 128)]


def whole(ref):
    n, m = ref.shape[:2]
    return jnp.concatenate([ref[:, h].reshape(8 * n, 128) for h in range(m)], axis=1)


def row_of(x, j):
    return jnp.broadcast_to(x[j : j + 1, :], x.shape)


def lane_of(x, at):
    return jnp.take_along_axis(x, at, axis=1)


def eight_pivots(k, base, a, r, inv):
    sub = lax.broadcasted_iota(jnp.int32, (8, 128), 0)
    lane = lax.broadcasted_iota(jnp.int32, (8, 128), 1)
    rel = [lane + (128 * h - 8 * k) for h in range(2)]
    inside = [(x >= 0) & (x < 8) for x in rel]
    c = k // 16
    start = 8 * lax.rem(k, 16)
    ats = [jnp.zeros((8, 128), jnp.int32) + (start + j) for j in range(8)]
    d = a[k, c]
    cols = [lane_of(d, at) for at in ats]
    work = [jnp.where(inside[h], (rel[h] == sub).astype(F32), a[k, h]) for h in range(2)] + [d]
    outs = [jnp.zeros((8, 128), F32) for _ in work]
    for j in range(8):
        here = sub == j
        root = lax.rsqrt(row_of(cols[j], j))
        scaled = cols[j] * root
        for m in range(j + 1, 8):
            term = row_of(cols[m], j) * root
            cols[m] = jnp.where(here, term * root, cols[m] - scaled * term)
        for w in range(3):
            term = row_of(work[w], j) * root
            outs[w] = jnp.where(here, term, outs[w])
            rest = work[w] - scaled * term
            work[w] = rest if w == 2 else jnp.where(here, term * root, rest)
    for h in range(2):
        r[k, h] = jnp.where(rel[h] >= 8, outs[h], jnp.where(inside[h] & (rel[h] >= sub), outs[2], 0.0))
        inv[k, h] = jnp.where(rel[h] <= sub, outs[h], 0.0)
    rows = [[row_of(work[h], j) for j in range(8)] for h in range(2)]
    source = [a[base + g, c] for g in range(8)]
    new = [[jnp.where(inside[h], 0.0, a[base + g, h]) for h in range(2)] for g in range(8)]
    for j in range(8):
        for g in range(8):
            multiplier = lane_of(source[g], ats[j])
            for h in range(2):
                new[g][h] = new[g][h] - multiplier * rows[h][j]
    for g in range(8):
        for h in range(2):
            a[base + g, h] = new[g][h]


def take_out(s, a, r, inv):
    base = 8 * s
    rows = lambda ref, h: ref[pl.ds(base, 8), h].reshape(64, 128)
    right = []
    for h in range(2):
        col = lax.broadcasted_iota(jnp.int32, (64, 128), 1) + 128 * h
        right.append(jnp.where(col < 64 * (s + 1), rows(inv, h), rows(r, h)))
    right = jnp.concatenate(right, axis=1)
    for half in range((s + 1) // 2, 2):
        product = tiled(dot(rows(r, half).T, right))
        for h in range(2):
            col = lax.broadcasted_iota(jnp.int32, (16, 8, 128), 2) + 128 * h
            old = a[pl.ds(16 * half, 16), h]
            a[pl.ds(16 * half, 16), h] = jnp.where((col >= 64 * s) & (col < 64 * (s + 1)), 0.0, old) - product[h]


def factor_part(eighth, a, r, inv):
    s = eighth // 2

    def step(i, carry):
        eight_pivots(4 * eighth + i, 8 * s, a, r, inv)
        return carry

    lax.fori_loop(0, 4, step, 0)
    if eighth % 2 and s < 3:
        take_out(s, a, r, inv)


def split(x):
    high = x.astype(jnp.bfloat16)
    return high, (x - high.astype(F32)).astype(jnp.bfloat16)


def split3(x):
    high = x.astype(jnp.bfloat16)
    rest = x - high.astype(F32)
    middle = rest.astype(jnp.bfloat16)
    return high, middle, (rest - middle.astype(F32)).astype(jnp.bfloat16)


def main_kernel(
    panel, trailing, block_high, block_low, rfactor, projected, weight_high, weight_low, held,
    block, a, inv, r, load_sem, side_send, side_recv, met, *rest
):
    p = Place()
    g = Reduction(p, rest[:12], True)
    t = [Reduction(p, rest[12 + 12 * q : 24 + 12 * q], False) for q in range(2)]

    owns = [
        pltpu.make_async_copy(panel.at[:, pl.ds(128 * q, 128)], block.at[p.x, q], load_sem.at[q]) for q in range(2)
    ]
    for own in owns:
        own.start()
    load = pltpu.make_async_copy(trailing, held, load_sem.at[2])

    beside = {axis: [p.at(**{axis: d}) for d in (1, size - 1)] for axis, size in (("y", 4), ("z", 8), ("x", 4))}
    barrier = pltpu.get_barrier_semaphore()
    for peer in [p.at(core=1)] + beside["y"] + beside["z"] + beside["x"]:
        pl.semaphore_signal(barrier, inc=1, device_id=peer, device_id_type=MESH)
    pl.semaphore_wait(barrier, 7)

    def tell(axis, at):
        for peer in beside[axis]:
            pl.semaphore_signal(met.at[at], inc=1, device_id=peer, device_id_type=MESH)

    def hear(at):
        pl.semaphore_wait(met.at[at], 2)

    for at, axis in enumerate(("y", "x", "z")):
        tell(axis, at)
    for own in owns:
        own.wait()
    load.start()

    steps = (1, 3)
    def side_copy(source, q, start, count, side, to):
        rows = block.at[source, q, pl.ds(start, count)]
        send(rows, rows, side_send.at[0], side_recv.at[to], p.at(x=steps[side]))

    def direct(to, q, n, start=0, count=256):
        for side in range(2):
            side_copy(p.x, q, 256 * (n if side == 0 else 1 - n) + start, count, side, to)

    def wait(at):
        like = block.at[0, 0]
        pltpu.make_async_copy(like, like, side_recv.at[at]).wait()

    def relay(to, q, at):
        wait(at)
        for side in range(2):
            side_copy(lax.rem(p.x + steps[1 - side], 4), q, 256 * side, 256, side, to)

    def add_cross(q, step, first=False, columns=(0, 1, 2, 3)):
        x = lax.rem(p.x + step, 4)
        right = held[pl.ds(512 * x, 512), 128 * columns[0] : 128 * columns[-1] + 128]
        for h, term in zip(columns, tiled(dot(block[x, q].T, right))):
            t[q].part[:, h] = term if first else t[q].part[:, h] + term

    direct(0, 0, 0)
    direct(1, 0, 1)
    mine = jnp.concatenate([block[p.x, q] for q in range(2)], axis=1)
    for h, tile in enumerate(tiled(dot(mine.T, mine))):
        g.part[:, h] = tile
    g.start_core()
    hear(0)
    hear(2)
    tell("z", 3)
    g.start_y()
    hear(3)
    tell("z", 4)
    load.wait()
    add_cross(0, 0, True)
    relay(2, 0, 0)
    direct(3, 1, 0, 0, 128)
    hear(4)
    hear(1)
    g.start_z()
    add_cross(1, 0, True)
    wait(1)
    add_cross(0, 1)
    add_cross(0, 3)
    g.start_x()
    direct(3, 1, 0, 128, 128)
    direct(4, 1, 1)
    wait(2)
    add_cross(0, 2)
    t[0].start_core()
    t[0].start_plane()
    g.start_gather()
    relay(5, 1, 3)
    wait(4)
    add_cross(1, 1)
    add_cross(1, 3)
    t[0].start_gather()
    wait(5)
    add_cross(1, 2, False, (0, 1))
    t[1].start_core(0, 2)
    add_cross(1, 2, False, (2, 3))
    t[1].start_core(2, 2)
    g.start_gather_core()
    t[1].start_plane()
    g.finish()
    a[...] = g.full[...]
    factor_part(0, a, r, inv)
    factor_part(1, a, r, inv)
    factor_part(2, a, r, inv)
    factor_part(3, a, r, inv)
    factor_part(4, a, r, inv)
    t[1].start_gather()
    for x in range(4):
        for q in range(2):
            at = (pl.ds(512 * x, 512), pl.ds(128 * q, 128))
            block_high[at], block_low[at] = split(block[x, q])
    factor_part(5, a, r, inv)
    t[0].start_gather_core()
    factor_part(6, a, r, inv)
    factor_part(7, a, r, inv)
    rfactor[...] = whole(r)
    inverse = whole(inv)
    square = dot(inverse.T, inverse)
    t[0].finish()
    upper = whole(t[0].full)
    projected[...] = dot(inverse[:, :128], upper)
    weight = dot(square[:, :128], upper)
    high, middle, low = split3(jnp.concatenate([square[:, 128:], inverse[128:, 128:]], axis=0))
    left = jnp.concatenate([high, middle], axis=1), jnp.concatenate([high, low], axis=1)
    t[1].start_gather_core()
    t[1].finish()
    high, middle, low = split3(whole(t[1].full))
    mul = functools.partial(jnp.dot, preferred_element_type=F32)
    twice = lambda a, b: jnp.concatenate([a, b], axis=0)
    product = mul(left[0], twice(high, high)) + (mul(left[0], twice(middle, middle)) + mul(left[1], twice(low, high)))
    weight_high[...], weight_low[...] = split(weight + product[:256])
    projected[128:, :] = projected[128:, :] + product[256:]
    sent = block.at[pl.ds(0, 3)]
    pltpu.make_async_copy(sent, sent, side_send.at[0]).wait()
    for reduction in (g, *t):
        reduction.drain()


def scratch(groups, across, sends, receives):
    tiles = lambda *shape: pltpu.VMEM((*shape, 8, 128), F32)
    return [
        tiles(groups, across), tiles(groups // 2, across), tiles(groups // 2, across), tiles(3, groups // 8, across),
        tiles(groups // 8, across), tiles(7), tiles(len(PLANE)), tiles(), tiles(4), tiles(groups, across),
        pltpu.SemaphoreType.DMA((sends,)), pltpu.SemaphoreType.DMA((receives,)),
    ]


def main_part(panel, trailing):
    inner = pl.BlockSpec(memory_space=pltpu.VMEM)
    halves = pltpu.VMEM((32, 2, 8, 128), F32)
    return pl.pallas_call(
        main_kernel,
        out_shape=(
            jax.ShapeDtypeStruct((2048, 256), jnp.bfloat16),
            jax.ShapeDtypeStruct((2048, 256), jnp.bfloat16),
            jax.ShapeDtypeStruct((256, 256), F32),
            jax.ShapeDtypeStruct((256, 512), F32),
            jax.ShapeDtypeStruct((256, 512), jnp.bfloat16),
            jax.ShapeDtypeStruct((256, 512), jnp.bfloat16),
            jax.ShapeDtypeStruct((2048, 512), F32),
        ),
        in_specs=[pl.BlockSpec(memory_space=pltpu.HBM)] * 2,
        out_specs=(inner,) * 7,
        scratch_shapes=[
            pltpu.VMEM((4, 2, 512, 128), F32),
            halves,
            halves,
            halves,
            pltpu.SemaphoreType.DMA((3,)),
            pltpu.SemaphoreType.DMA((1,)),
            pltpu.SemaphoreType.DMA((6,)),
            pltpu.SemaphoreType.REGULAR((5,)),
            *scratch(32, 2, 6, 9),
            *scratch(16, 4, 4, 7),
            *scratch(16, 4, 4, 7),
        ],
        compiler_params=pltpu.CompilerParams(collective_id=0, has_side_effects=True, vmem_limit_bytes=40 << 20),
    )(panel, trailing)


ROWS = 256


def update_kernel(held, high, low, weight_high, weight_low, rfactor, projected, rfactor_out, projected_out, updated, tiles, sems):
    n = 2048 // ROWS
    copies = [
        pltpu.make_async_copy(rfactor, rfactor_out, sems.at[n]),
        pltpu.make_async_copy(projected, projected_out, sems.at[n + 1]),
    ]
    for copy in copies:
        copy.start()
    mul = functools.partial(jnp.dot, preferred_element_type=F32)
    for i in range(n):
        rows = pl.ds(ROWS * i, ROWS)
        x = high[rows, :]
        product = mul(x, weight_high[...]) + (mul(x, weight_low[...]) + mul(low[rows, :], weight_high[...]))
        tiles[i] = held[rows, :] - product
        copy = pltpu.make_async_copy(tiles.at[i], updated.at[rows], sems.at[i])
        copy.start()
        copies.append(copy)
    for copy in copies:
        copy.wait()


def update(*operands):
    inner, outer = pl.BlockSpec(memory_space=pltpu.VMEM), pl.BlockSpec(memory_space=pltpu.HBM)
    return pl.pallas_call(
        update_kernel,
        out_shape=(
            jax.ShapeDtypeStruct((256, 256), F32),
            jax.ShapeDtypeStruct((256, 512), F32),
            jax.ShapeDtypeStruct((2048, 512), F32),
        ),
        in_specs=[inner] * 7,
        out_specs=(outer,) * 3,
        scratch_shapes=[pltpu.VMEM((2048 // ROWS, ROWS, 512), F32), pltpu.SemaphoreType.DMA((2048 // ROWS + 2,))],
        compiler_params=pltpu.CompilerParams(vmem_limit_bytes=24 << 20),
    )(*operands)


def shards(panel, trailing):
    outside = [pltpu.with_memory_space_constraint(x, pltpu.HBM) for x in (panel, trailing)]
    high, low, rfactor, projected, weight_high, weight_low, held = main_part(*outside)
    return update(held, high, low, weight_high, weight_low, rfactor, projected)


def solution(mesh):
    return jax.shard_map(
        shards,
        mesh=mesh,
        in_specs=(P(("rows", "cols"), None), P("rows", "cols")),
        out_specs=(P(), P(None, "cols"), P("rows", "cols")),
        check_vma=False,
    )
```
